128 devices in a mesh: groups: 4 (over x, y), tm: 16 (over z), rows: 2 (over core).
Axes of the slice: x: 2, y: 2, z: 16, core: 2. Of those that a mesh axis runs over, the one named last changes fastest.
The devices are a block of a 8x8x16 slice.
Arguments:
- iterate: float32 [128, 512, 512], P(('groups', 'tm'), 'rows'), parts along dimension 0, may hold values from -6 to 6
- forcing: float32 [128, 512, 512], P(('groups', 'tm'), 'rows'), parts along dimension 0, may hold values from -18 to 18
- initial_state: float32 [2048, 512], P(('groups', 'rows')), parts along dimension 0, may hold values from -6 to 6
- diffusivity: float32 [2048, 512], P(('groups', 'rows')), parts along dimension 0, may hold values from 0.5 to 4
Outputs:
- updated: float32 [128, 512, 512], P(('groups', 'tm'), 'rows'), parts along dimension 0
- residual_rms: float32 [128], P(('groups', 'tm')), parts along dimension 0
The draws below stay inside these ranges and needn't reach their ends.
There are 4 independent parts, one for each index of `groups`. The reference program is written for one: setup_inputs(seed, part) draws one part's arguments, and reference() takes and returns one part's arrays. A program takes and returns all parts, laid end to end along the dimension named above; each array names one. Nothing has to cross between parts.
All inputs are finite; a program needn't handle non-finite values.
Results may differ from the reference program's by a relative error of at most 0.0003.
Values sent between devices are 32-bit elements; how exact they have to be, the bound alone decides.
A program may use at most 64 MiB of HBM per device.

```python
import math
import jax
import jax.numpy as jnp
from jax import lax

NX = 512
NY = 512
CG_ITERS = 3
L = 32


def draw_forcing(key, part):
    dims_all = (L, NX, NY)
    return jax.random.truncated_normal(jax.random.fold_in(key, 17), -6.0, 6.0, dims_all, jnp.float32)


def steps_of(rng, shape, pieces, low, high):
    gain = 1.0
    for dim, parts in pieces:
        draws = jax.random.uniform(jax.random.fold_in(jax.random.fold_in(rng, 6), dim), (parts,), jnp.float32, low / len(pieces), high / len(pieces))
        gain = gain * jnp.repeat(jnp.exp(draws), shape[dim] // parts).reshape((-1,) + (1,) * (len(shape) - 1 - dim))
    return gain


def centred(stream_key, extent, width, reach, shards=(), kind=jnp.bfloat16):
    result = width * jax.random.normal(stream_key, extent, jnp.float32)
    if shards:
        result = result * steps_of(stream_key, extent, shards, -0.22, 0.18)
    return jnp.clip(result, -reach, reach).astype(kind)


def setup_inputs(seed: int = 0, part: int = 0) -> dict:
    streams_of = jax.random.split(jax.random.key(seed), 5)
    own_keys = jax.random.split(jax.random.fold_in(streams_of[4], part), 5)
    iterate = centred(own_keys[0], (L, NX, NY), 1.0, 6.0, ((0, 16), (1, 2)), jnp.float32)
    forcing = draw_forcing(jax.random.fold_in(jax.random.fold_in(streams_of[4], part), 71), part)
    initial_state = centred(own_keys[2], (NX, NY), 1.0, 6.0, ((0, 2),), jnp.float32)
    diffusivity = jnp.clip(jnp.exp(math.log(4.0) - 2.0794415 * jax.random.uniform(own_keys[3], (NX, NY), jnp.float32) ** steps_of(own_keys[3], (NX, NY), ((0, 2),), -0.2, 0.2)), 0.5, 4.0)
    return dict(iterate=iterate, forcing=forcing, initial_state=initial_state, diffusivity=diffusivity)


circulant_alpha = 0.05
time_step = 0.5
rms_eps = 1e-06

def phase_table(first_index, second_index, length):
    product = first_index[:, None] * second_index[None, :] % length
    return 2.0 * jnp.pi / length * product.astype(jnp.float32)

def faces_from(padded_rows):
    centre = padded_rows[1:-1]
    columns = jnp.pad(centre, ((0, 0), (1, 1)), mode='edge')
    north_face = 0.5 * (centre + padded_rows[:-2])
    south_face = 0.5 * (centre + padded_rows[2:])
    west_face = 0.5 * (centre + columns[:, :-2])
    east_face = 0.5 * (centre + columns[:, 2:])
    return (north_face, south_face, west_face, east_face)

def apply_faces(padded_rows, weights):
    north_face, south_face, west_face, east_face = weights
    centre = padded_rows[..., 1:-1, :]
    lead_pad = [(0, 0)] * (centre.ndim - 1)
    columns = jnp.pad(centre, lead_pad + [(1, 1)])
    return (north_face + south_face + west_face + east_face) * centre - north_face * padded_rows[..., :-2, :] - south_face * padded_rows[..., 2:, :] - west_face * columns[..., :-2] - east_face * columns[..., 2:]

def pad_rows(values):
    lead_pad = [(0, 0)] * (values.ndim - 2)
    return jnp.pad(values, lead_pad + [(1, 1), (0, 0)])

def apply_shifted(values, real_shift, imag_shift, weights, orientation):
    spread = time_step * apply_faces(pad_rows(values), weights)
    swapped = jnp.stack([-values[1], values[0]])
    return real_shift * values + orientation * imag_shift * swapped + spread

def normal_solve(rhs_values, real_shift, imag_shift, weights):

    def freq_norm(values):
        return lax.optimization_barrier(jnp.sum(values * values, axis=(0, 2, 3)))

    def expand(values):
        return values[None, :, None, None]
    solution = jnp.zeros_like(rhs_values)
    remain = rhs_values
    normal = apply_shifted(remain, real_shift, imag_shift, weights, -1.0)
    gamma_now = freq_norm(normal)
    search = normal
    for iteration in range(CG_ITERS):
        image_now = apply_shifted(search, real_shift, imag_shift, weights, 1.0)
        step_rate = gamma_now / freq_norm(image_now)
        solution = solution + expand(step_rate) * search
        if iteration + 1 < CG_ITERS:
            remain = remain - expand(step_rate) * image_now
            normal = apply_shifted(remain, real_shift, imag_shift, weights, -1.0)
            gamma_next = freq_norm(normal)
            search = normal + expand(gamma_next / gamma_now) * search
            gamma_now = gamma_next
    return solution

def reference(iterate, forcing, initial_state, diffusivity):
    length = iterate.shape[0]
    cell_count = NX * NY
    faces = faces_from(jnp.pad(diffusivity, ((1, 1), (0, 0)), mode='edge'))
    previous = jnp.concatenate([initial_state[None], iterate[:-1]], axis=0)
    residual = time_step * forcing + previous - iterate - time_step * apply_faces(pad_rows(iterate), faces)
    residual_rms = jnp.sqrt(lax.optimization_barrier(jnp.sum(residual * residual, axis=(1, 2))) / cell_count + rms_eps)
    all_index = jnp.arange(length, dtype=jnp.int32)
    log_alpha = jnp.log(jnp.float32(circulant_alpha))
    growth = jnp.exp(log_alpha * all_index.astype(jnp.float32) / length)
    scaled = residual * growth[:, None, None]
    angles = phase_table(all_index, all_index, length)
    flat_cells = scaled.reshape(length, -1)
    spectrum_real = jnp.dot(jnp.cos(angles), flat_cells, precision=lax.Precision.HIGHEST, preferred_element_type=jnp.float32)
    spectrum_imag = jnp.dot(-jnp.sin(angles), flat_cells, precision=lax.Precision.HIGHEST, preferred_element_type=jnp.float32)
    spectrum = jnp.stack([spectrum_real, spectrum_imag]).reshape(2, length, NX, NY)
    root_alpha = jnp.exp(log_alpha / length)
    freq_angle = 2.0 * jnp.pi / length * all_index.astype(jnp.float32)
    real_shift = (1.0 - root_alpha * jnp.cos(freq_angle))[:, None, None]
    imag_shift = (root_alpha * jnp.sin(freq_angle))[:, None, None]
    solution = normal_solve(spectrum, real_shift, imag_shift, faces)
    flat_real = solution[0].reshape(length, -1)
    flat_imag = solution[1].reshape(length, -1)
    correction = jnp.dot(jnp.cos(angles) / length, flat_real, precision=lax.Precision.HIGHEST, preferred_element_type=jnp.float32) - jnp.dot(jnp.sin(angles) / length, flat_imag, precision=lax.Precision.HIGHEST, preferred_element_type=jnp.float32)
    correction = correction.reshape(length, NX, NY)
    updated = iterate + correction / growth[:, None, None]
    return (updated, residual_rms)
```

```python
import functools

import jax
import jax.numpy as jnp
import numpy as np
from jax import lax
from jax.experimental import pallas as pl
from jax.experimental.pallas import tpu as pltpu
from jax.sharding import PartitionSpec as P

circulant_alpha = 0.05
time_step = 0.5
rms_eps = 1e-06
MESH = pl.DeviceIdType.MESH


def rfft_list(x):
    n = len(x)
    if n == 1:
        return [(x[0], None)]
    even, odd = rfft_list(x[0::2]), rfft_list(x[1::2])
    half = n // 2
    out = [None] * (half + 1)
    out[0] = (even[0][0] + odd[0][0], None)
    out[half] = (even[0][0] - odd[0][0], None)
    for k in range(1, half // 2 + 1):
        if 2 * k == half:
            out[k] = (even[k][0], -odd[k][0])
            continue
        angle = 2.0 * np.pi * k / n
        cos, sin = float(np.cos(angle)), float(np.sin(angle))
        o_re, o_im = odd[k]
        if 8 * k == n:
            t_re, t_im = (o_re + o_im) * cos, (o_im - o_re) * cos
        else:
            t_re, t_im = o_re * cos + o_im * sin, o_im * cos - o_re * sin
        e_re, e_im = even[k]
        out[k] = (e_re + t_re, e_im + t_im)
        out[half - k] = (e_re - t_re, t_im - e_im)
    return out


def irfft_list(freq):
    half = len(freq) - 1
    n = 2 * half
    if n == 2:
        return [freq[0][0] + freq[1][0], freq[0][0] - freq[1][0]]
    even, odd = [None] * (half // 2 + 1), [None] * (half // 2 + 1)
    even[0] = (freq[0][0] + freq[half][0], None)
    odd[0] = (freq[0][0] - freq[half][0], None)
    for k in range(1, half // 2 + 1):
        if 2 * k == half:
            even[k] = (freq[k][0] + freq[k][0], None)
            odd[k] = (-(freq[k][1] + freq[k][1]), None)
            continue
        angle = 2.0 * np.pi * k / n
        cos, sin = float(np.cos(angle)), float(np.sin(angle))
        a_re, a_im = freq[k]
        b_re, b_im = freq[half - k]
        even[k] = (a_re + b_re, a_im - b_im)
        d_re, d_im = a_re - b_re, a_im + b_im
        if 8 * k == n:
            odd[k] = ((d_re - d_im) * cos, (d_re + d_im) * cos)
        else:
            odd[k] = (d_re * cos - d_im * sin, d_im * cos + d_re * sin)
    even_out, odd_out = irfft_list(even), irfft_list(odd)
    out = [None] * n
    out[0::2], out[1::2] = even_out, odd_out
    return out


def two_sum(a, b):
    s = a + b
    v = s - a
    return s, (a - (s - v)) + (b - v)


def quick_sum(a, b):
    s = a + b
    return s, b - (s - a)


def split(a):
    t = 4097.0 * a
    hi = t - (t - a)
    return hi, a - hi


def two_prod(a, b):
    p = a * b
    ah, al = split(a)
    bh, bl = split(b)
    return p, ((ah * bh - p) + ah * bl + al * bh) + al * bl


def pair_add(x, y):
    s, e = two_sum(x[0], y[0])
    return quick_sum(s, e + (x[1] + y[1]))


def pair_neg(x):
    return (-x[0], -x[1])


def pair_mul(x, y):
    p, e = two_prod(x[0], y[0])
    return quick_sum(p, e + (x[0] * y[1] + x[1] * y[0]))


def pair_div(x, y):
    q = x[0] / y[0]
    rest = pair_add(x, pair_neg(pair_mul((q, jnp.zeros_like(q)), y)))
    return quick_sum(q, rest[0] / y[0])


def krylov_weights(mu):
    one = (jnp.ones_like(mu[0][0]), jnp.zeros_like(mu[0][0]))
    zero = jnp.zeros_like(mu[0][0])
    inv0 = pair_div(one, mu[0])
    t1 = pair_div(mu[0], mu[1])
    t2 = pair_mul(t1, t1)
    t3 = pair_mul(t2, t1)
    t4 = pair_mul(t2, t2)
    t5 = pair_mul(t4, t1)
    m2, m3, m4, m5 = (
        pair_mul(pair_mul(mu[k], inv0), t) for k, t in ((2, t2), (3, t3), (4, t4), (5, t5))
    )
    tiny = 2.0**-32
    gain0 = pair_add(m2, pair_neg(one))
    den1 = pair_add(m3, pair_neg(pair_mul(m2, m2)))
    ok1 = (gain0[0] > tiny) & (den1[0] > tiny * m3[0])

    def kept(ok, x, other):
        return (jnp.where(ok, x[0], other), jnp.where(ok, x[1], 0.0))

    rate1 = kept(ok1, pair_div(kept(ok1, gain0, 0.0), kept(ok1, den1, 1.0)), 0.0)
    mid = pair_add(one, pair_mul(rate1, m2))
    inner = pair_add(pair_add(m2, pair_neg(pair_mul(mid, m3))), pair_mul(rate1, m4))
    size = m2[0] + mid[0] * m3[0] + rate1[0] * m4[0]
    ok2 = ok1 & (inner[0] > tiny * size)
    gamma2 = pair_mul(rate1, kept(ok2, inner, 0.0))
    gain1 = pair_div(gamma2, kept(ok1, gain0, 1.0))
    base = pair_add(one, pair_mul(gain1, m2))
    slope = pair_add(mid, gain1)
    inner2 = pair_add(
        pair_add(pair_mul(base, m3), pair_neg(pair_mul(slope, m4))), pair_mul(rate1, m5)
    )
    size2 = base[0] * m3[0] + slope[0] * m4[0] + rate1[0] * m5[0]
    ok3 = ok2 & (inner2[0] > tiny * size2)
    ratio = kept(ok2, inner, 0.0)
    rate2 = pair_div(ratio, kept(ok3, inner2, 1.0))
    rate2 = jnp.where(ok3, rate2[0], zero)
    w0 = mid[0] + rate2 * base[0]
    w1 = -(rate1[0] + rate2 * slope[0])
    w2 = rate2 * rate1[0]
    return w0 * t1[0], w1 * t2[0], w2 * t3[0]


def kernel(
    count,
    cells,
    it_hbm,
    fo_hbm,
    init_hbm,
    di_hbm,
    tab,
    out_ref,
    rms_ref,
    u_ext,
    force,
    before,
    d_ext,
    res,
    by_cell,
    spec,
    v0_ref,
    v1_ref,
    v2_ref,
    corr,
    back,
    weights,
    mom,
    coef,
    ar_send,
    ar_all,
    sq_send,
    sq_recv,
    load_sem,
    prev_sem,
    rim_send,
    rim_recv,
    a_send,
    a_recv,
    h_send,
    h_recv,
    m_send,
    m_recv,
    b_send,
    b_recv,
):
    t = lax.axis_index("tm")
    c = lax.axis_index("rows")
    me = c * count + t
    total = 2 * count
    length = 2 * count
    pairs = length // 2
    rows = force.shape[1]
    cols = force.shape[2]
    slab = rows // count
    tiles = cols // 128

    def pos(i):
        return {"tm": lax.rem(i, count), "rows": i // count}

    barrier = pltpu.get_barrier_semaphore()

    def greet(k, carry):
        pl.semaphore_signal(
            barrier, inc=1, device_id=pos(lax.rem(me + k, total)), device_id_type=MESH
        )
        return carry

    lax.fori_loop(1, total, greet, 0)

    loads = [
        pltpu.make_async_copy(di_hbm, d_ext.at[pl.ds(16, rows)], load_sem.at[0]),
        pltpu.make_async_copy(it_hbm, u_ext.at[:, pl.ds(8, rows)], load_sem.at[1]),
        pltpu.make_async_copy(fo_hbm, force, load_sem.at[2]),
    ]
    for load in loads:
        load.start()
    u_ext[:, pl.ds(pl.multiple_of(c * (rows + 8), 8), 8), :] = jnp.zeros((2, 8, cols), jnp.float32)
    pl.semaphore_wait(barrier, total - 1)

    partner = {"rows": 1 - c}
    rims = [
        pltpu.make_async_remote_copy(
            src_ref=di_hbm.at[pl.ds(pl.multiple_of((1 - c) * (rows - 16), 8), 16)],
            dst_ref=d_ext.at[pl.ds(pl.multiple_of(c * (rows + 16), 8), 16)],
            send_sem=rim_send.at[0],
            recv_sem=rim_recv.at[0],
            device_id=partner,
            device_id_type=MESH,
        ),
        pltpu.make_async_remote_copy(
            src_ref=it_hbm.at[:, pl.ds(pl.multiple_of((1 - c) * (rows - 8), 8), 8)],
            dst_ref=u_ext.at[:, pl.ds(pl.multiple_of(c * (rows + 8), 8), 8)],
            send_sem=rim_send.at[1],
            recv_sem=rim_recv.at[1],
            device_id=partner,
            device_id_type=MESH,
        ),
    ]
    for rim in rims:
        rim.start()

    onward = pltpu.make_async_remote_copy(
        src_ref=it_hbm.at[1],
        dst_ref=before,
        send_sem=prev_sem.at[0],
        recv_sem=prev_sem.at[1],
        device_id={"tm": lax.rem(t + 1, count)},
        device_id_type=MESH,
    )
    first = pltpu.make_async_copy(init_hbm, before, prev_sem.at[2])

    @pl.when(t < count - 1)
    def _():
        onward.start()

    @pl.when(t == 0)
    def _():
        first.start()

    for load in loads:
        load.wait()
    edge = jnp.where(c == 0, d_ext[16:24, :][:1], d_ext[rows + 8 : rows + 16, :][7:8])
    d_ext[pl.ds(pl.multiple_of(c * (rows + 16), 8), 16), :] = jnp.broadcast_to(edge, (16, cols))
    for rim in rims:
        rim.wait_recv()

    def lane_of(shape):
        return lax.broadcasted_iota(jnp.int32, shape, 1)

    def residual(step, dest):
        start = pl.multiple_of(dest * slab, slab)
        tall = slab + 16
        u = u_ext[step, pl.ds(start, tall), :]
        d = d_ext[pl.ds(pl.multiple_of(start + 8, 8), tall), :]
        lane = lane_of((slab, cols))
        mid = slice(8, slab + 8)
        uc, dc = u[mid], d[mid]
        u_n, u_s = pltpu.roll(u, 1, 0)[mid], pltpu.roll(u, tall - 1, 0)[mid]
        d_n, d_s = pltpu.roll(d, 1, 0)[mid], pltpu.roll(d, tall - 1, 0)[mid]
        u_w = jnp.where(lane == 0, 0.0, pltpu.roll(uc, 1, 1))
        u_e = jnp.where(lane == cols - 1, 0.0, pltpu.roll(uc, cols - 1, 1))
        d_w = jnp.where(lane == 0, dc, pltpu.roll(dc, 1, 1))
        d_e = jnp.where(lane == cols - 1, dc, pltpu.roll(dc, cols - 1, 1))
        spread = (
            (dc + d_n) * (uc - u_n)
            + (dc + d_s) * (uc - u_s)
            + (dc + d_w) * (uc - u_w)
            + (dc + d_e) * (uc - u_e)
        )
        if step == 0:
            prev = before[pl.ds(start, slab), :]
        else:
            prev = u_ext[step - 1, pl.ds(pl.multiple_of(start + 8, 8), slab), :]
        value = time_step * force[step, pl.ds(start, slab), :] + prev - uc
        return value - (0.5 * time_step) * spread

    def squares(value):
        sq = value * value
        folded = sq[0:8]
        for i in range(1, slab // 8):
            folded = folded + sq[8 * i : 8 * i + 8]
        total_sq = folded[:, 0:128]
        for i in range(1, tiles):
            total_sq = total_sq + folded[:, 128 * i : 128 * i + 128]
        return total_sq

    def peer(k):
        far = count // 2 - (k + 1) // 2
        return lax.rem(t + jnp.where(lax.rem(k, 2) == 1, far, count - far), count)

    def forward(step, k):
        dest = peer(k)
        block = pl.ds(pl.multiple_of(dest * slab, slab), slab)
        return pltpu.make_async_remote_copy(
            src_ref=res.at[step, block],
            dst_ref=by_cell.at[2 * t + step],
            send_sem=a_send.at[step, k],
            recv_sem=a_recv.at[step, t],
            device_id={"tm": dest},
            device_id_type=MESH,
        )

    for step in (1, 0):
        if step == 0:

            @pl.when(t > 0)
            def _():
                onward.wait_recv()

            @pl.when(t == 0)
            def _():
                first.wait()

        growth = tab[2 * t + step]

        def send_one(k, acc):
            dest = peer(k)
            value = residual(step, dest)
            res[step, pl.ds(pl.multiple_of(dest * slab, slab), slab), :] = value * growth
            forward(step, k).start()
            return acc + squares(value)

        acc = lax.fori_loop(0, count - 1, send_one, jnp.zeros((8, 128), jnp.float32))
        value = residual(step, t)
        by_cell[2 * t + step] = value * growth
        sq_send[step] = acc + squares(value)

    sq_copy = pltpu.make_async_remote_copy(
        src_ref=sq_send,
        dst_ref=sq_recv,
        send_sem=rim_send.at[2],
        recv_sem=rim_recv.at[2],
        device_id=partner,
        device_id_type=MESH,
    )
    sq_copy.start()

    d = d_ext[pl.ds(pl.multiple_of(t * slab, slab), slab + 32), :]
    tall = slab + 16
    mid = slice(8, slab + 24)
    dc = d[mid]
    lane = lane_of((tall, cols))
    quarter = 0.5 * time_step
    w_n = quarter * (dc + pltpu.roll(d, 1, 0)[mid])
    w_s = quarter * (dc + pltpu.roll(d, slab + 31, 0)[mid])
    w_w = quarter * (dc + jnp.where(lane == 0, dc, pltpu.roll(dc, 1, 1)))
    w_e = quarter * (dc + jnp.where(lane == cols - 1, dc, pltpu.roll(dc, cols - 1, 1)))
    weights[0] = w_n + w_s + w_w + w_e
    weights[1] = w_n
    weights[2] = w_s
    weights[3] = jnp.where(lane == 0, 0.0, w_w)
    weights[4] = jnp.where(lane == cols - 1, 0.0, w_e)

    def arrived(k, carry):
        source = peer(k)
        for step in (0, 1):
            pltpu.make_async_remote_copy(
                src_ref=res.at[step, pl.ds(0, slab)],
                dst_ref=by_cell.at[2 * source + step],
                send_sem=a_send.at[step, k],
                recv_sem=a_recv.at[step, source],
                device_id={"tm": source},
                device_id_type=MESH,
            ).wait_recv()
        return carry

    lax.fori_loop(0, count - 1, arrived, 0)

    row_tiles = slab // 8

    def transform(p, carry):
        r = pl.multiple_of((p // tiles) * 8, 8)
        q = pl.multiple_of(lax.rem(p, tiles) * 128, 128)
        x = [by_cell[n, pl.ds(r, 8), pl.ds(q, 128)] for n in range(length)]
        f = rfft_list(x)
        here = (pl.ds(pl.multiple_of(r + 8, 8), 8), pl.ds(q, 128))
        spec[(0,) + here] = f[0][0]
        spec[(1,) + here] = f[pairs][0]
        for j in range(1, pairs):
            spec[(2 * j,) + here] = f[j][0]
            spec[(2 * j + 1,) + here] = f[j][1]
        return carry

    lax.fori_loop(0, row_tiles * tiles, transform, 0)

    north, south = pos(lax.rem(me + total - 1, total)), pos(lax.rem(me + 1, total))

    def halo(side, q):
        fields = pl.ds(2 * q, 2)
        if side == 0:
            src, dst, target = slab, 0, south
        else:
            src, dst, target = 8, slab + 8, north
        return pltpu.make_async_remote_copy(
            src_ref=spec.at[fields, pl.ds(src, 8)],
            dst_ref=spec.at[fields, pl.ds(dst, 8)],
            send_sem=h_send.at[side, q],
            recv_sem=h_recv.at[side, q],
            device_id=target,
            device_id_type=MESH,
        )

    def send_halo(q, carry):
        halo(0, q).start()
        halo(1, q).start()
        return carry

    lax.fori_loop(0, pairs, send_halo, 0)

    top = jnp.where(me == 0, 0.0, 1.0)
    bottom = jnp.where(me == total - 1, 0.0, 1.0)
    n_tr = row_tiles + 2
    sub = lax.broadcasted_iota(jnp.int32, (8, cols), 0)

    def spread_of(v, wanted):
        down = [pltpu.roll(x, 1, 0) for x in v]
        up = [pltpu.roll(x, 7, 0) for x in v]
        out = {}
        for i in wanted:
            v_n = jnp.where(sub == 0, down[max(i - 1, 0)], down[i])
            v_s = jnp.where(sub == 7, up[min(i + 1, n_tr - 1)], up[i])
            here = slice(8 * i, 8 * i + 8)
            out[i] = (
                weights[0, here, :] * v[i]
                - weights[1, here, :] * v_n
                - weights[2, here, :] * v_s
                - weights[3, here, :] * pltpu.roll(v[i], 1, 1)
                - weights[4, here, :] * pltpu.roll(v[i], cols - 1, 1)
            )
        return out

    def clip(i, x):
        if i == 0:
            return x * top
        if i == n_tr - 1:
            return x * bottom
        return x

    inner = range(1, n_tr - 1)

    def folded(v):
        acc = None
        for i in inner:
            sq = v[i] * v[i]
            for k in range(tiles):
                part = sq[:, 128 * k : 128 * k + 128]
                acc = part if acc is None else acc + part
        return jnp.sum(acc, axis=0, keepdims=True)

    def solve(q, carry):
        halo(0, q).wait_recv()
        halo(1, q).wait_recv()
        a_re, a_im, b = tab[2 * length + q], tab[2 * length + pairs + q], tab[2 * length + 2 * pairs + q]
        v = [
            [clip(i, spec[2 * q + part, 8 * i : 8 * i + 8, :]) for i in range(n_tr)]
            for part in (0, 1)
        ]
        for order in range(6):
            wanted = inner if order == 5 else range(n_tr)
            sign = b if order % 2 == 0 else -b
            k_re, k_im = spread_of(v[0], wanted), spread_of(v[1], wanted)
            new_re, new_im = [None] * n_tr, [None] * n_tr
            for i in wanted:
                new_re[i] = clip(i, a_re * v[0][i] + sign * v[1][i] + k_re[i])
                new_im[i] = clip(i, a_im * v[1][i] - sign * v[0][i] + k_im[i])
            v = [new_re, new_im]
            mom[2 * order, pl.ds(q, 1), :] = folded(v[0])
            mom[2 * order + 1, pl.ds(q, 1), :] = folded(v[1])
            if order % 2 == 0:
                keep = (v0_ref, v1_ref, v2_ref)[order // 2]
                for part in (0, 1):
                    for i in inner:
                        keep[2 * q + part, 8 * i - 8 : 8 * i, :] = v[part][i]
        return carry

    lax.fori_loop(0, pairs, solve, 0)

    row = lax.broadcasted_iota(jnp.int32, (pairs, 128), 0)
    lane8 = lax.broadcasted_iota(jnp.int32, (8, 128), 1)
    row8 = lax.broadcasted_iota(jnp.int32, (8, 128), 0)
    packed = [jnp.zeros((8, 128), jnp.float32), jnp.zeros((8, 128), jnp.float32)]

    def slot(k, g):
        return lane8 == (16 * row8 + 2 * k + g if g < 2 else 16 * k + 12)

    for k in range(6):
        re, im = mom[2 * k], mom[2 * k + 1]
        both = jnp.where(row == 0, re, re + im)
        for g in range(3):
            x = both[8 * g : 8 * g + 8] if g < 2 else im[0:8]
            big = 256.0 * jnp.max(x, axis=1, keepdims=True)
            hi = (x + big) - big
            lo = x - hi
            where = slot(k, g) if g < 2 else slot(k, g) & (row8 == 0)
            packed[0] = jnp.where(where, jnp.sum(hi, axis=1, keepdims=True), packed[0])
            packed[1] = jnp.where(where, jnp.sum(lo, axis=1, keepdims=True), packed[1])
    mine = jnp.concatenate([jnp.sum(x, axis=0, keepdims=True) for x in packed], axis=1)
    ar_send[...] = mine
    ar_all[me] = mine

    def share(k):
        return pltpu.make_async_remote_copy(
            src_ref=ar_send,
            dst_ref=ar_all.at[me],
            send_sem=m_send.at[k],
            recv_sem=m_recv.at[me],
            device_id=pos(lax.rem(me + k, total)),
            device_id_type=MESH,
        )

    def share_one(k, carry):
        share(k).start()
        return carry

    lax.fori_loop(1, total, share_one, 0)

    def shared(k, carry):
        source = lax.rem(me + k, total)
        pltpu.make_async_remote_copy(
            src_ref=ar_send,
            dst_ref=ar_all.at[source],
            send_sem=m_send.at[k],
            recv_sem=m_recv.at[source],
            device_id=pos(source),
            device_id_type=MESH,
        ).wait_recv()
        return carry

    lax.fori_loop(1, total, shared, 0)
    sums = [(ar_all[i][:, 0:128], ar_all[i][:, 128:256]) for i in range(total)]
    while len(sums) > 1:
        sums = [pair_add(sums[2 * i], sums[2 * i + 1]) for i in range(len(sums) // 2)]
    whole = [jnp.broadcast_to(x, (8, 128)) for x in sums[0]]
    mu = []
    for k in range(6):
        sides = []
        for x in whole:
            groups = [
                jnp.broadcast_to(
                    jnp.sum(jnp.where(slot(k, g), x, 0.0), axis=1, keepdims=True), (8, 128)
                )
                for g in range(3)
            ]
            sides.append(jnp.concatenate(groups, axis=0))
        mu.append(tuple(sides))
    for k, w in enumerate(krylov_weights(mu)):
        coef[k, 0] = w[0:pairs]
        coef[k, 1] = jnp.where(row == 0, w[pairs : pairs + 1], w[0:pairs])

    def restore(p, carry):
        r = pl.multiple_of((p // tiles) * 8, 8)
        q = pl.multiple_of(lax.rem(p, tiles) * 128, 128)
        here = (pl.ds(r, 8), pl.ds(q, 128))

        def field(f):
            j, part = f // 2, f % 2
            out = coef[0, part, j : j + 1, :] * v0_ref[(f,) + here]
            out = out + coef[1, part, j : j + 1, :] * v1_ref[(f,) + here]
            return out + coef[2, part, j : j + 1, :] * v2_ref[(f,) + here]

        freq = [(field(0), None)]
        freq += [(field(2 * j), field(2 * j + 1)) for j in range(1, pairs)]
        freq += [(field(1), None)]
        for n, x in enumerate(irfft_list(freq)):
            corr[(n,) + here] = x * tab[length + n]
        return carry

    lax.fori_loop(0, row_tiles * tiles, restore, 0)

    own = pl.ds(pl.multiple_of(t * slab, slab), slab)

    def send_back(k, carry):
        dest = peer(k)
        pltpu.make_async_remote_copy(
            src_ref=corr.at[pl.ds(2 * dest, 2)],
            dst_ref=back.at[:, own],
            send_sem=b_send.at[k],
            recv_sem=b_recv.at[t],
            device_id={"tm": dest},
            device_id_type=MESH,
        ).start()
        return carry

    lax.fori_loop(0, count - 1, send_back, 0)

    sq_copy.wait()
    rms = jnp.sqrt(
        jnp.sum(jnp.sum(sq_send[...] + sq_recv[...], axis=2, keepdims=True), axis=1, keepdims=True) / cells
        + rms_eps
    )
    rms_ref[...] = jnp.broadcast_to(rms[:, 0], (2, 128))

    def final(source, piece):
        block = pl.ds(pl.multiple_of(source * slab, slab), slab)
        ahead = pl.ds(pl.multiple_of(source * slab + 8, 8), slab)
        out_ref[:, block, :] = u_ext[:, ahead, :] + piece

    final(t, corr[pl.ds(2 * t, 2)])

    def returned(k, carry):
        source = peer(k)
        block = pl.ds(pl.multiple_of(source * slab, slab), slab)
        pltpu.make_async_remote_copy(
            src_ref=corr.at[pl.ds(0, 2)],
            dst_ref=back.at[:, block],
            send_sem=b_send.at[k],
            recv_sem=b_recv.at[source],
            device_id={"tm": source},
            device_id_type=MESH,
        ).wait_recv()
        final(source, back[:, block, :])
        return carry

    lax.fori_loop(0, count - 1, returned, 0)

    for rim in rims:
        rim.wait_send()

    @pl.when(t < count - 1)
    def _():
        onward.wait_send()

    def drain_peers(k, carry):
        forward(0, k).wait_send()
        forward(1, k).wait_send()
        pltpu.make_async_remote_copy(
            src_ref=corr.at[pl.ds(0, 2)],
            dst_ref=back.at[:, own],
            send_sem=b_send.at[k],
            recv_sem=b_recv.at[t],
            device_id={"tm": peer(k)},
            device_id_type=MESH,
        ).wait_send()
        return carry

    lax.fori_loop(0, count - 1, drain_peers, 0)

    def drain_halo(q, carry):
        halo(0, q).wait_send()
        halo(1, q).wait_send()
        return carry

    lax.fori_loop(0, pairs, drain_halo, 0)

    def drain_share(k, carry):
        share(k).wait_send()
        return carry

    lax.fori_loop(1, total, drain_share, 0)


def tables(length):
    pairs = length // 2
    n = np.arange(length)
    growth = np.exp(np.log(circulant_alpha) * n / length)
    root = np.exp(np.log(circulant_alpha) / length)
    j = np.arange(pairs)
    a_re = 1.0 - root * np.cos(2.0 * np.pi * j / length)
    a_im = a_re.copy()
    a_im[0] = 1.0 + root
    b = root * np.sin(2.0 * np.pi * j / length)
    return np.concatenate([growth, 1.0 / (length * growth), a_re, a_im, b]).astype(np.float32)


def shards(iterate, forcing, initial_state, diffusivity):
    steps, rows, cols = iterate.shape
    count = lax.axis_size("tm")
    halves = lax.axis_size("rows")
    length = steps * count
    assert steps == 2 and halves == 2
    slab = rows // count
    pairs = length // 2
    total = 2 * count
    cells = rows * halves * cols
    f32 = jnp.float32
    vmem = pltpu.VMEM
    dma = pltpu.SemaphoreType.DMA
    hbm = pl.BlockSpec(memory_space=pl.ANY)
    updated, rms = pl.pallas_call(
        functools.partial(kernel, count, cells),
        out_shape=(
            jax.ShapeDtypeStruct((steps, rows, cols), f32),
            jax.ShapeDtypeStruct((steps, 128), f32),
        ),
        in_specs=[hbm] * 4 + [pl.BlockSpec(memory_space=pltpu.SMEM)],
        out_specs=(pl.BlockSpec(memory_space=vmem), pl.BlockSpec(memory_space=vmem)),
        scratch_shapes=[
            vmem((steps, rows + 16, cols), f32),
            vmem((steps, rows, cols), f32),
            vmem((rows, cols), f32),
            vmem((rows + 32, cols), f32),
            vmem((steps, rows, cols), f32),
            vmem((length, slab, cols), f32),
            vmem((length, slab + 16, cols), f32),
            vmem((length, slab, cols), f32),
            vmem((length, slab, cols), f32),
            vmem((length, slab, cols), f32),
            vmem((length, slab, cols), f32),
            vmem((steps, rows, cols), f32),
            vmem((5, slab + 16, cols), f32),
            vmem((12, pairs, 128), f32),
            vmem((3, 2, pairs, 128), f32),
            vmem((1, 256), f32),
            vmem((total, 1, 256), f32),
            vmem((2, 8, 128), f32),
            vmem((2, 8, 128), f32),
            dma((3,)),
            dma((3,)),
            dma((3,)),
            dma((3,)),
            dma((2, count)),
            dma((2, count)),
            dma((2, pairs)),
            dma((2, pairs)),
            dma((total,)),
            dma((total,)),
            dma((count,)),
            dma((count,)),
        ],
        compiler_params=pltpu.CompilerParams(collective_id=0, has_side_effects=True),
        name="paradiag",
    )(iterate, forcing, initial_state, diffusivity, jnp.asarray(tables(length)))
    return updated, rms[:, 0]


def solution(mesh):
    placed = (
        P(("groups", "tm"), "rows", None),
        P(("groups", "tm"), "rows", None),
        P(("groups", "rows"), None),
        P(("groups", "rows"), None),
    )
    return jax.shard_map(
        shards,
        mesh=mesh,
        in_specs=placed,
        out_specs=(P(("groups", "tm"), "rows", None), P(("groups", "tm"))),
        check_vma=False,
    )
```

```python
import functools

import jax
import jax.numpy as jnp
import numpy as np
from jax import lax
from jax.experimental import pallas as pl
from jax.experimental.pallas import tpu as pltpu
from jax.sharding import PartitionSpec as P

circulant_alpha = 0.05
time_step = 0.5
rms_eps = 1e-06
MESH = pl.DeviceIdType.MESH


def rfft_list(x):
    n = len(x)
    if n == 1:
        return [(x[0], None)]
    even, odd = rfft_list(x[0::2]), rfft_list(x[1::2])
    half = n // 2
    out = [None] * (half + 1)
    out[0] = (even[0][0] + odd[0][0], None)
    out[half] = (even[0][0] - odd[0][0], None)
    for k in range(1, half // 2 + 1):
        if 2 * k == half:
            out[k] = (even[k][0], -odd[k][0])
            continue
        angle = 2.0 * np.pi * k / n
        cos, sin = float(np.cos(angle)), float(np.sin(angle))
        o_re, o_im = odd[k]
        if 8 * k == n:
            t_re, t_im = (o_re + o_im) * cos, (o_im - o_re) * cos
        else:
            t_re, t_im = o_re * cos + o_im * sin, o_im * cos - o_re * sin
        e_re, e_im = even[k]
        out[k] = (e_re + t_re, e_im + t_im)
        out[half - k] = (e_re - t_re, t_im - e_im)
    return out


def irfft_list(freq):
    half = len(freq) - 1
    n = 2 * half
    if n == 2:
        return [freq[0][0] + freq[1][0], freq[0][0] - freq[1][0]]
    even, odd = [None] * (half // 2 + 1), [None] * (half // 2 + 1)
    even[0] = (freq[0][0] + freq[half][0], None)
    odd[0] = (freq[0][0] - freq[half][0], None)
    for k in range(1, half // 2 + 1):
        if 2 * k == half:
            even[k] = (freq[k][0] + freq[k][0], None)
            odd[k] = (-(freq[k][1] + freq[k][1]), None)
            continue
        angle = 2.0 * np.pi * k / n
        cos, sin = float(np.cos(angle)), float(np.sin(angle))
        a_re, a_im = freq[k]
        b_re, b_im = freq[half - k]
        even[k] = (a_re + b_re, a_im - b_im)
        d_re, d_im = a_re - b_re, a_im + b_im
        if 8 * k == n:
            odd[k] = ((d_re - d_im) * cos, (d_re + d_im) * cos)
        else:
            odd[k] = (d_re * cos - d_im * sin, d_im * cos + d_re * sin)
    even_out, odd_out = irfft_list(even), irfft_list(odd)
    out = [None] * n
    out[0::2], out[1::2] = even_out, odd_out
    return out


def two_sum(a, b):
    s = a + b
    v = s - a
    return s, (a - (s - v)) + (b - v)


def quick_sum(a, b):
    s = a + b
    return s, b - (s - a)


def split(a):
    t = 4097.0 * a
    hi = t - (t - a)
    return hi, a - hi


def two_prod(a, b):
    p = a * b
    ah, al = split(a)
    bh, bl = split(b)
    return p, ((ah * bh - p) + ah * bl + al * bh) + al * bl


def pair_add(x, y):
    s, e = two_sum(x[0], y[0])
    return quick_sum(s, e + (x[1] + y[1]))


def pair_neg(x):
    return (-x[0], -x[1])


def pair_mul(x, y):
    p, e = two_prod(x[0], y[0])
    return quick_sum(p, e + (x[0] * y[1] + x[1] * y[0]))


def pair_div(x, y):
    q = x[0] / y[0]
    rest = pair_add(x, pair_neg(pair_mul((q, jnp.zeros_like(q)), y)))
    return quick_sum(q, rest[0] / y[0])


def krylov_weights(mu):
    one = (jnp.ones_like(mu[0][0]), jnp.zeros_like(mu[0][0]))
    zero = jnp.zeros_like(mu[0][0])
    inv0 = pair_div(one, mu[0])
    t1 = pair_div(mu[0], mu[1])
    t2 = pair_mul(t1, t1)
    t3 = pair_mul(t2, t1)
    t4 = pair_mul(t2, t2)
    t5 = pair_mul(t4, t1)
    m2, m3, m4, m5 = (
        pair_mul(pair_mul(mu[k], inv0), t) for k, t in ((2, t2), (3, t3), (4, t4), (5, t5))
    )
    tiny = 2.0**-32
    gain0 = pair_add(m2, pair_neg(one))
    den1 = pair_add(m3, pair_neg(pair_mul(m2, m2)))
    ok1 = (gain0[0] > tiny) & (den1[0] > tiny * m3[0])

    def kept(ok, x, other):
        return (jnp.where(ok, x[0], other), jnp.where(ok, x[1], 0.0))

    rate1 = kept(ok1, pair_div(kept(ok1, gain0, 0.0), kept(ok1, den1, 1.0)), 0.0)
    mid = pair_add(one, pair_mul(rate1, m2))
    inner = pair_add(pair_add(m2, pair_neg(pair_mul(mid, m3))), pair_mul(rate1, m4))
    size = m2[0] + mid[0] * m3[0] + rate1[0] * m4[0]
    ok2 = ok1 & (inner[0] > tiny * size)
    gamma2 = pair_mul(rate1, kept(ok2, inner, 0.0))
    gain1 = pair_div(gamma2, kept(ok1, gain0, 1.0))
    base = pair_add(one, pair_mul(gain1, m2))
    slope = pair_add(mid, gain1)
    inner2 = pair_add(
        pair_add(pair_mul(base, m3), pair_neg(pair_mul(slope, m4))), pair_mul(rate1, m5)
    )
    size2 = base[0] * m3[0] + slope[0] * m4[0] + rate1[0] * m5[0]
    ok3 = ok2 & (inner2[0] > tiny * size2)
    ratio = kept(ok2, inner, 0.0)
    rate2 = pair_div(ratio, kept(ok3, inner2, 1.0))
    rate2 = jnp.where(ok3, rate2[0], zero)
    w0 = mid[0] + rate2 * base[0]
    w1 = -(rate1[0] + rate2 * slope[0])
    w2 = rate2 * rate1[0]
    return w0 * t1[0], w1 * t2[0], w2 * t3[0]


def kernel(
    count,
    cells,
    it_hbm,
    fo_hbm,
    init_hbm,
    di_hbm,
    tab,
    out_ref,
    rms_ref,
    u_ext,
    force,
    before,
    d_ext,
    res,
    by_cell,
    spec,
    v0_ref,
    v1_ref,
    v2_ref,
    corr,
    back,
    weights,
    mom,
    coef,
    ar_send,
    ar_all,
    sq_send,
    sq_recv,
    load_sem,
    prev_sem,
    rim_send,
    rim_recv,
    a_send,
    a_recv,
    h_send,
    h_recv,
    m_send,
    m_recv,
    b_send,
    b_recv,
    from_left,
    from_right,
):
    t = lax.axis_index("tm")
    c = lax.axis_index("rows")
    me = c * count + t
    total = 2 * count
    length = 2 * count
    pairs = length // 2
    rows = force.shape[1]
    cols = force.shape[2]
    slab = rows // count
    tiles = cols // 128

    def pos(i):
        return {"tm": lax.rem(i, count), "rows": i // count}

    barrier = pltpu.get_barrier_semaphore()

    right, left = {"tm": lax.rem(t + 1, count)}, {"tm": lax.rem(t + count - 1, count)}
    partner = {"rows": 1 - c}
    for neighbour in (left, right, partner):
        pl.semaphore_signal(barrier, inc=1, device_id=neighbour, device_id_type=MESH)

    loads = [
        pltpu.make_async_copy(di_hbm, d_ext.at[pl.ds(16, rows)], load_sem.at[0]),
        pltpu.make_async_copy(it_hbm, u_ext.at[:, pl.ds(8, rows)], load_sem.at[1]),
        pltpu.make_async_copy(fo_hbm, force, load_sem.at[2]),
    ]
    for load in loads:
        load.start()
    u_ext[:, pl.ds(pl.multiple_of(c * (rows + 8), 8), 8), :] = jnp.zeros((2, 8, cols), jnp.float32)
    pl.semaphore_wait(barrier, 3)

    onward = pltpu.make_async_remote_copy(
        src_ref=it_hbm.at[1],
        dst_ref=before,
        send_sem=prev_sem.at[0],
        recv_sem=prev_sem.at[1],
        device_id=right,
        device_id_type=MESH,
    )
    first = pltpu.make_async_copy(init_hbm, before, prev_sem.at[2])

    @pl.when(t < count - 1)
    def _():
        onward.start()

    @pl.when(t == 0)
    def _():
        first.start()

    rims = [
        pltpu.make_async_remote_copy(
            src_ref=di_hbm.at[pl.ds(pl.multiple_of((1 - c) * (rows - 16), 8), 16)],
            dst_ref=d_ext.at[pl.ds(pl.multiple_of(c * (rows + 16), 8), 16)],
            send_sem=rim_send.at[0],
            recv_sem=rim_recv.at[0],
            device_id=partner,
            device_id_type=MESH,
        ),
        pltpu.make_async_remote_copy(
            src_ref=it_hbm.at[:, pl.ds(pl.multiple_of((1 - c) * (rows - 8), 8), 8)],
            dst_ref=u_ext.at[:, pl.ds(pl.multiple_of(c * (rows + 8), 8), 8)],
            send_sem=rim_send.at[1],
            recv_sem=rim_recv.at[1],
            device_id=partner,
            device_id_type=MESH,
        ),
    ]
    for rim in rims:
        rim.start()

    for load in loads:
        load.wait()
    edge = jnp.where(c == 0, d_ext[16:24, :][:1], d_ext[rows + 8 : rows + 16, :][7:8])
    d_ext[pl.ds(pl.multiple_of(c * (rows + 16), 8), 16), :] = jnp.broadcast_to(edge, (16, cols))
    for rim in rims:
        rim.wait_recv()

    def lane_of(shape):
        return lax.broadcasted_iota(jnp.int32, shape, 1)

    def residual(step, dest):
        start = pl.multiple_of(dest * slab, slab)
        tall = slab + 16
        u = u_ext[step, pl.ds(start, tall), :]
        d = d_ext[pl.ds(pl.multiple_of(start + 8, 8), tall), :]
        lane = lane_of((slab, cols))
        mid = slice(8, slab + 8)
        uc, dc = u[mid], d[mid]
        u_n, u_s = pltpu.roll(u, 1, 0)[mid], pltpu.roll(u, tall - 1, 0)[mid]
        d_n, d_s = pltpu.roll(d, 1, 0)[mid], pltpu.roll(d, tall - 1, 0)[mid]
        u_w = jnp.where(lane == 0, 0.0, pltpu.roll(uc, 1, 1))
        u_e = jnp.where(lane == cols - 1, 0.0, pltpu.roll(uc, cols - 1, 1))
        d_w = jnp.where(lane == 0, dc, pltpu.roll(dc, 1, 1))
        d_e = jnp.where(lane == cols - 1, dc, pltpu.roll(dc, cols - 1, 1))
        spread = (
            (dc + d_n) * (uc - u_n)
            + (dc + d_s) * (uc - u_s)
            + (dc + d_w) * (uc - u_w)
            + (dc + d_e) * (uc - u_e)
        )
        if step == 0:
            prev = before[pl.ds(start, slab), :]
        else:
            prev = u_ext[step - 1, pl.ds(pl.multiple_of(start + 8, 8), slab), :]
        value = time_step * force[step, pl.ds(start, slab), :] + prev - uc
        return value - (0.5 * time_step) * spread

    def squares(value):
        sq = value * value
        folded = sq[0:8]
        for i in range(1, slab // 8):
            folded = folded + sq[8 * i : 8 * i + 8]
        total_sq = folded[:, 0:128]
        for i in range(1, tiles):
            total_sq = total_sq + folded[:, 128 * i : 128 * i + 128]
        return total_sq

    def peer(k):
        far = count // 2 - (k + 1) // 2
        return lax.rem(t + jnp.where(lax.rem(k, 2) == 1, far, count - far), count)

    def forward(step, dest):
        block = pl.ds(pl.multiple_of(dest * slab, slab), slab)
        return pltpu.make_async_remote_copy(
            src_ref=res.at[step, block],
            dst_ref=by_cell.at[2 * t + step],
            send_sem=a_send.at[step, dest],
            recv_sem=a_recv.at[step, t],
            device_id={"tm": dest},
            device_id_type=MESH,
        )

    def send_one(step, dest, acc):
        value = residual(step, dest)
        res[step, pl.ds(pl.multiple_of(dest * slab, slab), slab), :] = value * tab[2 * t + step]
        forward(step, dest).start()
        return acc + squares(value)

    def keep_own(step, acc):
        value = residual(step, t)
        by_cell[2 * t + step] = value * tab[2 * t + step]
        sq_send[step] = acc + squares(value)

    def pass_tokens():
        pl.semaphore_signal(from_left, inc=1, device_id=right, device_id_type=MESH)
        pl.semaphore_signal(from_right, inc=1, device_id=left, device_id_type=MESH)

    def widen(k, acc):
        pass_tokens()
        acc = send_one(1, lax.rem(t + k, count), acc)
        acc = send_one(1, lax.rem(t + count - k, count), acc)
        pl.semaphore_wait(from_left, 1)
        pl.semaphore_wait(from_right, 1)
        return acc

    acc = lax.fori_loop(1, count // 2, widen, jnp.zeros((8, 128), jnp.float32))
    pass_tokens()
    acc = send_one(1, lax.rem(t + count // 2, count), acc)
    keep_own(1, acc)

    @pl.when(t > 0)
    def _():
        onward.wait_recv()

    @pl.when(t == 0)
    def _():
        first.wait()

    acc = lax.fori_loop(
        0, count - 1, lambda k, acc: send_one(0, peer(k), acc), jnp.zeros((8, 128), jnp.float32)
    )
    keep_own(0, acc)
    pl.semaphore_wait(from_left, 1)
    pl.semaphore_wait(from_right, 1)

    sq_copy = pltpu.make_async_remote_copy(
        src_ref=sq_send,
        dst_ref=sq_recv,
        send_sem=rim_send.at[2],
        recv_sem=rim_recv.at[2],
        device_id=partner,
        device_id_type=MESH,
    )
    sq_copy.start()

    d = d_ext[pl.ds(pl.multiple_of(t * slab, slab), slab + 32), :]
    tall = slab + 16
    mid = slice(8, slab + 24)
    dc = d[mid]
    lane = lane_of((tall, cols))
    quarter = 0.5 * time_step
    w_n = quarter * (dc + pltpu.roll(d, 1, 0)[mid])
    w_s = quarter * (dc + pltpu.roll(d, slab + 31, 0)[mid])
    w_w = quarter * (dc + jnp.where(lane == 0, dc, pltpu.roll(dc, 1, 1)))
    w_e = quarter * (dc + jnp.where(lane == cols - 1, dc, pltpu.roll(dc, cols - 1, 1)))
    weights[0] = w_n + w_s + w_w + w_e
    weights[1] = w_n
    weights[2] = w_s
    weights[3] = jnp.where(lane == 0, 0.0, w_w)
    weights[4] = jnp.where(lane == cols - 1, 0.0, w_e)

    def arrived(k, carry):
        source = peer(k)
        for step in (0, 1):
            pltpu.make_async_remote_copy(
                src_ref=res.at[step, pl.ds(0, slab)],
                dst_ref=by_cell.at[2 * source + step],
                send_sem=a_send.at[step, source],
                recv_sem=a_recv.at[step, source],
                device_id={"tm": source},
                device_id_type=MESH,
            ).wait_recv()
        return carry

    lax.fori_loop(0, count - 1, arrived, 0)

    row_tiles = slab // 8

    def transform(p, carry):
        r = pl.multiple_of((p // tiles) * 8, 8)
        q = pl.multiple_of(lax.rem(p, tiles) * 128, 128)
        x = [by_cell[n, pl.ds(r, 8), pl.ds(q, 128)] for n in range(length)]
        f = rfft_list(x)
        here = (pl.ds(pl.multiple_of(r + 8, 8), 8), pl.ds(q, 128))
        spec[(0,) + here] = f[0][0]
        spec[(1,) + here] = f[pairs][0]
        for j in range(1, pairs):
            spec[(2 * j,) + here] = f[j][0]
            spec[(2 * j + 1,) + here] = f[j][1]
        return carry

    lax.fori_loop(0, row_tiles * tiles, transform, 0)

    north, south = pos(lax.rem(me + total - 1, total)), pos(lax.rem(me + 1, total))

    def halo(side, q):
        fields = pl.ds(2 * q, 2)
        if side == 0:
            src, dst, target = slab, 0, south
        else:
            src, dst, target = 8, slab + 8, north
        return pltpu.make_async_remote_copy(
            src_ref=spec.at[fields, pl.ds(src, 8)],
            dst_ref=spec.at[fields, pl.ds(dst, 8)],
            send_sem=h_send.at[side, q],
            recv_sem=h_recv.at[side, q],
            device_id=target,
            device_id_type=MESH,
        )

    def send_halo(q, carry):
        halo(0, q).start()
        halo(1, q).start()
        return carry

    lax.fori_loop(0, pairs, send_halo, 0)

    top = jnp.where(me == 0, 0.0, 1.0)
    bottom = jnp.where(me == total - 1, 0.0, 1.0)
    n_tr = row_tiles + 2
    sub = lax.broadcasted_iota(jnp.int32, (8, cols), 0)

    def spread_of(v, wanted):
        down = [pltpu.roll(x, 1, 0) for x in v]
        up = [pltpu.roll(x, 7, 0) for x in v]
        out = {}
        for i in wanted:
            v_n = jnp.where(sub == 0, down[max(i - 1, 0)], down[i])
            v_s = jnp.where(sub == 7, up[min(i + 1, n_tr - 1)], up[i])
            here = slice(8 * i, 8 * i + 8)
            out[i] = (
                weights[0, here, :] * v[i]
                - weights[1, here, :] * v_n
                - weights[2, here, :] * v_s
                - weights[3, here, :] * pltpu.roll(v[i], 1, 1)
                - weights[4, here, :] * pltpu.roll(v[i], cols - 1, 1)
            )
        return out

    def clip(i, x):
        if i == 0:
            return x * top
        if i == n_tr - 1:
            return x * bottom
        return x

    inner = range(1, n_tr - 1)

    def folded(v):
        acc = None
        for i in inner:
            sq = v[i] * v[i]
            for k in range(tiles):
                part = sq[:, 128 * k : 128 * k + 128]
                acc = part if acc is None else acc + part
        return jnp.sum(acc, axis=0, keepdims=True)

    def solve(q, carry):
        halo(0, q).wait_recv()
        halo(1, q).wait_recv()
        a_re, a_im, b = tab[2 * length + q], tab[2 * length + pairs + q], tab[2 * length + 2 * pairs + q]
        v = [
            [clip(i, spec[2 * q + part, 8 * i : 8 * i + 8, :]) for i in range(n_tr)]
            for part in (0, 1)
        ]
        for order in range(6):
            wanted = inner if order == 5 else range(n_tr)
            sign = b if order % 2 == 0 else -b
            k_re, k_im = spread_of(v[0], wanted), spread_of(v[1], wanted)
            new_re, new_im = [None] * n_tr, [None] * n_tr
            for i in wanted:
                new_re[i] = clip(i, a_re * v[0][i] + sign * v[1][i] + k_re[i])
                new_im[i] = clip(i, a_im * v[1][i] - sign * v[0][i] + k_im[i])
            v = [new_re, new_im]
            mom[2 * order, pl.ds(q, 1), :] = folded(v[0])
            mom[2 * order + 1, pl.ds(q, 1), :] = folded(v[1])
            if order % 2 == 0:
                keep = (v0_ref, v1_ref, v2_ref)[order // 2]
                for part in (0, 1):
                    for i in inner:
                        keep[2 * q + part, 8 * i - 8 : 8 * i, :] = v[part][i]
        return carry

    lax.fori_loop(0, pairs, solve, 0)

    row = lax.broadcasted_iota(jnp.int32, (pairs, 128), 0)
    lane8 = lax.broadcasted_iota(jnp.int32, (8, 128), 1)
    row8 = lax.broadcasted_iota(jnp.int32, (8, 128), 0)
    packed = [jnp.zeros((8, 128), jnp.float32), jnp.zeros((8, 128), jnp.float32)]

    def slot(k, g):
        return lane8 == (16 * row8 + 2 * k + g if g < 2 else 16 * k + 12)

    for k in range(6):
        re, im = mom[2 * k], mom[2 * k + 1]
        both = jnp.where(row == 0, re, re + im)
        for g in range(3):
            x = both[8 * g : 8 * g + 8] if g < 2 else im[0:8]
            big = 256.0 * jnp.max(x, axis=1, keepdims=True)
            hi = (x + big) - big
            lo = x - hi
            where = slot(k, g) if g < 2 else slot(k, g) & (row8 == 0)
            packed[0] = jnp.where(where, jnp.sum(hi, axis=1, keepdims=True), packed[0])
            packed[1] = jnp.where(where, jnp.sum(lo, axis=1, keepdims=True), packed[1])
    mine = jnp.concatenate([jnp.sum(x, axis=0, keepdims=True) for x in packed], axis=1)
    ar_send[...] = mine
    ar_all[me] = mine

    def share(k):
        return pltpu.make_async_remote_copy(
            src_ref=ar_send,
            dst_ref=ar_all.at[me],
            send_sem=m_send.at[k],
            recv_sem=m_recv.at[me],
            device_id=pos(lax.rem(me + k, total)),
            device_id_type=MESH,
        )

    def share_one(k, carry):
        share(k).start()
        return carry

    lax.fori_loop(1, total, share_one, 0)

    def shared(k, carry):
        source = lax.rem(me + k, total)
        pltpu.make_async_remote_copy(
            src_ref=ar_send,
            dst_ref=ar_all.at[source],
            send_sem=m_send.at[k],
            recv_sem=m_recv.at[source],
            device_id=pos(source),
            device_id_type=MESH,
        ).wait_recv()
        return carry

    lax.fori_loop(1, total, shared, 0)
    sums = [(ar_all[i][:, 0:128], ar_all[i][:, 128:256]) for i in range(total)]
    while len(sums) > 1:
        sums = [pair_add(sums[2 * i], sums[2 * i + 1]) for i in range(len(sums) // 2)]
    whole = [jnp.broadcast_to(x, (8, 128)) for x in sums[0]]
    mu = []
    for k in range(6):
        sides = []
        for x in whole:
            groups = [
                jnp.broadcast_to(
                    jnp.sum(jnp.where(slot(k, g), x, 0.0), axis=1, keepdims=True), (8, 128)
                )
                for g in range(3)
            ]
            sides.append(jnp.concatenate(groups, axis=0))
        mu.append(tuple(sides))
    for k, w in enumerate(krylov_weights(mu)):
        coef[k, 0] = w[0:pairs]
        coef[k, 1] = jnp.where(row == 0, w[pairs : pairs + 1], w[0:pairs])

    def restore(p, carry):
        r = pl.multiple_of((p // tiles) * 8, 8)
        q = pl.multiple_of(lax.rem(p, tiles) * 128, 128)
        here = (pl.ds(r, 8), pl.ds(q, 128))

        def field(f):
            j, part = f // 2, f % 2
            out = coef[0, part, j : j + 1, :] * v0_ref[(f,) + here]
            out = out + coef[1, part, j : j + 1, :] * v1_ref[(f,) + here]
            return out + coef[2, part, j : j + 1, :] * v2_ref[(f,) + here]

        freq = [(field(0), None)]
        freq += [(field(2 * j), field(2 * j + 1)) for j in range(1, pairs)]
        freq += [(field(1), None)]
        for n, x in enumerate(irfft_list(freq)):
            corr[(n,) + here] = x * tab[length + n]
        return carry

    lax.fori_loop(0, row_tiles * tiles, restore, 0)

    own = pl.ds(pl.multiple_of(t * slab, slab), slab)

    def send_back(k, carry):
        dest = peer(k)
        pltpu.make_async_remote_copy(
            src_ref=corr.at[pl.ds(2 * dest, 2)],
            dst_ref=back.at[:, own],
            send_sem=b_send.at[k],
            recv_sem=b_recv.at[t],
            device_id={"tm": dest},
            device_id_type=MESH,
        ).start()
        return carry

    lax.fori_loop(0, count - 1, send_back, 0)

    sq_copy.wait()
    rms = jnp.sqrt(
        jnp.sum(jnp.sum(sq_send[...] + sq_recv[...], axis=2, keepdims=True), axis=1, keepdims=True) / cells
        + rms_eps
    )
    rms_ref[...] = jnp.broadcast_to(rms[:, 0], (2, 128))

    def final(source, piece):
        block = pl.ds(pl.multiple_of(source * slab, slab), slab)
        ahead = pl.ds(pl.multiple_of(source * slab + 8, 8), slab)
        out_ref[:, block, :] = u_ext[:, ahead, :] + piece

    final(t, corr[pl.ds(2 * t, 2)])

    def returned(k, carry):
        source = peer(k)
        block = pl.ds(pl.multiple_of(source * slab, slab), slab)
        pltpu.make_async_remote_copy(
            src_ref=corr.at[pl.ds(0, 2)],
            dst_ref=back.at[:, block],
            send_sem=b_send.at[k],
            recv_sem=b_recv.at[source],
            device_id={"tm": source},
            device_id_type=MESH,
        ).wait_recv()
        final(source, back[:, block, :])
        return carry

    lax.fori_loop(0, count - 1, returned, 0)

    for rim in rims:
        rim.wait_send()

    @pl.when(t < count - 1)
    def _():
        onward.wait_send()

    def drain_peers(k, carry):
        forward(0, peer(k)).wait_send()
        forward(1, peer(k)).wait_send()
        pltpu.make_async_remote_copy(
            src_ref=corr.at[pl.ds(0, 2)],
            dst_ref=back.at[:, own],
            send_sem=b_send.at[k],
            recv_sem=b_recv.at[t],
            device_id={"tm": peer(k)},
            device_id_type=MESH,
        ).wait_send()
        return carry

    lax.fori_loop(0, count - 1, drain_peers, 0)

    def drain_halo(q, carry):
        halo(0, q).wait_send()
        halo(1, q).wait_send()
        return carry

    lax.fori_loop(0, pairs, drain_halo, 0)

    def drain_share(k, carry):
        share(k).wait_send()
        return carry

    lax.fori_loop(1, total, drain_share, 0)


def tables(length):
    pairs = length // 2
    n = np.arange(length)
    growth = np.exp(np.log(circulant_alpha) * n / length)
    root = np.exp(np.log(circulant_alpha) / length)
    j = np.arange(pairs)
    a_re = 1.0 - root * np.cos(2.0 * np.pi * j / length)
    a_im = a_re.copy()
    a_im[0] = 1.0 + root
    b = root * np.sin(2.0 * np.pi * j / length)
    return np.concatenate([growth, 1.0 / (length * growth), a_re, a_im, b]).astype(np.float32)


def shards(iterate, forcing, initial_state, diffusivity):
    steps, rows, cols = iterate.shape
    count = lax.axis_size("tm")
    halves = lax.axis_size("rows")
    length = steps * count
    assert steps == 2 and halves == 2
    slab = rows // count
    pairs = length // 2
    total = 2 * count
    cells = rows * halves * cols
    f32 = jnp.float32
    vmem = pltpu.VMEM
    dma = pltpu.SemaphoreType.DMA
    hbm = pl.BlockSpec(memory_space=pl.ANY)
    updated, rms = pl.pallas_call(
        functools.partial(kernel, count, cells),
        out_shape=(
            vmem((steps, rows, cols), f32),
            vmem((steps, 128), f32),
        ),
        in_specs=[hbm] * 4 + [pl.BlockSpec(memory_space=pltpu.SMEM)],
        out_specs=(pl.BlockSpec(memory_space=vmem), pl.BlockSpec(memory_space=vmem)),
        scratch_shapes=[
            vmem((steps, rows + 16, cols), f32),
            vmem((steps, rows, cols), f32),
            vmem((rows, cols), f32),
            vmem((rows + 32, cols), f32),
            vmem((steps, rows, cols), f32),
            vmem((length, slab, cols), f32),
            vmem((length, slab + 16, cols), f32),
            vmem((length, slab, cols), f32),
            vmem((length, slab, cols), f32),
            vmem((length, slab, cols), f32),
            vmem((length, slab, cols), f32),
            vmem((steps, rows, cols), f32),
            vmem((5, slab + 16, cols), f32),
            vmem((12, pairs, 128), f32),
            vmem((3, 2, pairs, 128), f32),
            vmem((1, 256), f32),
            vmem((total, 1, 256), f32),
            vmem((2, 8, 128), f32),
            vmem((2, 8, 128), f32),
            dma((3,)),
            dma((3,)),
            dma((3,)),
            dma((3,)),
            dma((2, count)),
            dma((2, count)),
            dma((2, pairs)),
            dma((2, pairs)),
            dma((total,)),
            dma((total,)),
            dma((count,)),
            dma((count,)),
            pltpu.SemaphoreType.REGULAR,
            pltpu.SemaphoreType.REGULAR,
        ],
        compiler_params=pltpu.CompilerParams(collective_id=0, has_side_effects=True),
        name="paradiag",
    )(iterate, forcing, initial_state, diffusivity, jnp.asarray(tables(length)))
    return updated, rms[:, 0]


def solution(mesh):
    placed = (
        P(("groups", "tm"), "rows", None),
        P(("groups", "tm"), "rows", None),
        P(("groups", "rows"), None),
        P(("groups", "rows"), None),
    )
    return jax.shard_map(
        shards,
        mesh=mesh,
        in_specs=placed,
        out_specs=(P(("groups", "tm"), "rows", None), P(("groups", "tm"))),
        check_vma=False,
    )
```

```python
import functools

import jax
import jax.numpy as jnp
import numpy as np
from jax import lax
from jax.experimental import pallas as pl
from jax.experimental.pallas import tpu as pltpu
from jax.sharding import PartitionSpec as P

circulant_alpha = 0.05
time_step = 0.5
rms_eps = 1e-06
MESH = pl.DeviceIdType.MESH


def rfft_list(x):
    n = len(x)
    if n == 1:
        return [(x[0], None)]
    even, odd = rfft_list(x[0::2]), rfft_list(x[1::2])
    half = n // 2
    out = [None] * (half + 1)
    out[0] = (even[0][0] + odd[0][0], None)
    out[half] = (even[0][0] - odd[0][0], None)
    for k in range(1, half // 2 + 1):
        if 2 * k == half:
            out[k] = (even[k][0], -odd[k][0])
            continue
        angle = 2.0 * np.pi * k / n
        cos, sin = float(np.cos(angle)), float(np.sin(angle))
        o_re, o_im = odd[k]
        if 8 * k == n:
            t_re, t_im = (o_re + o_im) * cos, (o_im - o_re) * cos
        else:
            t_re, t_im = o_re * cos + o_im * sin, o_im * cos - o_re * sin
        e_re, e_im = even[k]
        out[k] = (e_re + t_re, e_im + t_im)
        out[half - k] = (e_re - t_re, t_im - e_im)
    return out


def irfft_list(freq):
    half = len(freq) - 1
    n = 2 * half
    if n == 2:
        return [freq[0][0] + freq[1][0], freq[0][0] - freq[1][0]]
    even, odd = [None] * (half // 2 + 1), [None] * (half // 2 + 1)
    even[0] = (freq[0][0] + freq[half][0], None)
    odd[0] = (freq[0][0] - freq[half][0], None)
    for k in range(1, half // 2 + 1):
        if 2 * k == half:
            even[k] = (freq[k][0] + freq[k][0], None)
            odd[k] = (-(freq[k][1] + freq[k][1]), None)
            continue
        angle = 2.0 * np.pi * k / n
        cos, sin = float(np.cos(angle)), float(np.sin(angle))
        a_re, a_im = freq[k]
        b_re, b_im = freq[half - k]
        even[k] = (a_re + b_re, a_im - b_im)
        d_re, d_im = a_re - b_re, a_im + b_im
        if 8 * k == n:
            odd[k] = ((d_re - d_im) * cos, (d_re + d_im) * cos)
        else:
            odd[k] = (d_re * cos - d_im * sin, d_im * cos + d_re * sin)
    even_out, odd_out = irfft_list(even), irfft_list(odd)
    out = [None] * n
    out[0::2], out[1::2] = even_out, odd_out
    return out


def two_sum(a, b):
    s = a + b
    v = s - a
    return s, (a - (s - v)) + (b - v)


def quick_sum(a, b):
    s = a + b
    return s, b - (s - a)


def split(a):
    t = 4097.0 * a
    hi = t - (t - a)
    return hi, a - hi


def two_prod(a, b):
    p = a * b
    ah, al = split(a)
    bh, bl = split(b)
    return p, ((ah * bh - p) + ah * bl + al * bh) + al * bl


def pair_add(x, y):
    s, e = two_sum(x[0], y[0])
    return quick_sum(s, e + (x[1] + y[1]))


def pair_neg(x):
    return (-x[0], -x[1])


def pair_mul(x, y):
    p, e = two_prod(x[0], y[0])
    return quick_sum(p, e + (x[0] * y[1] + x[1] * y[0]))


def pair_div(x, y):
    q = x[0] / y[0]
    rest = pair_add(x, pair_neg(pair_mul((q, jnp.zeros_like(q)), y)))
    return quick_sum(q, rest[0] / y[0])


def krylov_weights(mu):
    one = (jnp.ones_like(mu[0][0]), jnp.zeros_like(mu[0][0]))
    zero = jnp.zeros_like(mu[0][0])
    inv0 = pair_div(one, mu[0])
    t1 = pair_div(mu[0], mu[1])
    t2 = pair_mul(t1, t1)
    t3 = pair_mul(t2, t1)
    t4 = pair_mul(t2, t2)
    t5 = pair_mul(t4, t1)
    m2, m3, m4, m5 = (
        pair_mul(pair_mul(mu[k], inv0), t) for k, t in ((2, t2), (3, t3), (4, t4), (5, t5))
    )
    tiny = 2.0**-32
    gain0 = pair_add(m2, pair_neg(one))
    den1 = pair_add(m3, pair_neg(pair_mul(m2, m2)))
    ok1 = (gain0[0] > tiny) & (den1[0] > tiny * m3[0])

    def kept(ok, x, other):
        return (jnp.where(ok, x[0], other), jnp.where(ok, x[1], 0.0))

    rate1 = kept(ok1, pair_div(kept(ok1, gain0, 0.0), kept(ok1, den1, 1.0)), 0.0)
    mid = pair_add(one, pair_mul(rate1, m2))
    inner = pair_add(pair_add(m2, pair_neg(pair_mul(mid, m3))), pair_mul(rate1, m4))
    size = m2[0] + mid[0] * m3[0] + rate1[0] * m4[0]
    ok2 = ok1 & (inner[0] > tiny * size)
    gamma2 = pair_mul(rate1, kept(ok2, inner, 0.0))
    gain1 = pair_div(gamma2, kept(ok1, gain0, 1.0))
    base = pair_add(one, pair_mul(gain1, m2))
    slope = pair_add(mid, gain1)
    inner2 = pair_add(
        pair_add(pair_mul(base, m3), pair_neg(pair_mul(slope, m4))), pair_mul(rate1, m5)
    )
    size2 = base[0] * m3[0] + slope[0] * m4[0] + rate1[0] * m5[0]
    ok3 = ok2 & (inner2[0] > tiny * size2)
    ratio = kept(ok2, inner, 0.0)
    rate2 = pair_div(ratio, kept(ok3, inner2, 1.0))
    rate2 = jnp.where(ok3, rate2[0], zero)
    w0 = mid[0] + rate2 * base[0]
    w1 = -(rate1[0] + rate2 * slope[0])
    w2 = rate2 * rate1[0]
    return w0 * t1[0], w1 * t2[0], w2 * t3[0]


def kernel(
    count,
    cells,
    it_hbm,
    fo_hbm,
    init_hbm,
    di_hbm,
    tab,
    out_ref,
    rms_ref,
    u_ext,
    force,
    before,
    d_ext,
    res,
    by_cell,
    spec,
    v0_ref,
    v1_ref,
    v2_ref,
    xs,
    corr,
    back,
    weights,
    mom,
    coef,
    ar_send,
    ar_all,
    sq_send,
    sq_recv,
    load_sem,
    prev_sem,
    rim_send,
    rim_recv,
    a_send,
    a_recv,
    h_send,
    h_recv,
    x_send,
    x_recv,
    y_send,
    y_recv,
    m_send,
    m_recv,
    b_send,
    b_recv,
    from_left,
    from_right,
):
    t = lax.axis_index("tm")
    c = lax.axis_index("rows")
    length = 2 * count
    pairs = length // 2
    share = pairs // 2
    rows = force.shape[1]
    cols = force.shape[2]
    half = count // 2
    slab = rows // half
    piece = slab // 2
    tiles = cols // 128
    home = t // half
    place = lax.rem(t, half)

    barrier = pltpu.get_barrier_semaphore()

    right, left = {"tm": lax.rem(t + 1, count)}, {"tm": lax.rem(t + count - 1, count)}
    partner = {"rows": 1 - c}
    for neighbour in (left, right, partner):
        pl.semaphore_signal(barrier, inc=1, device_id=neighbour, device_id_type=MESH)

    loads = [
        pltpu.make_async_copy(di_hbm, d_ext.at[pl.ds(pl.multiple_of(16 + rows * c, 8), rows)], load_sem.at[0]),
        pltpu.make_async_copy(it_hbm, u_ext.at[:, pl.ds(8, rows)], load_sem.at[1]),
        pltpu.make_async_copy(fo_hbm, force, load_sem.at[2]),
    ]
    for load in loads:
        load.start()
    u_ext[:, pl.ds(pl.multiple_of(c * (rows + 8), 8), 8), :] = jnp.zeros((2, 8, cols), jnp.float32)
    pl.semaphore_wait(barrier, 3)

    onward = pltpu.make_async_remote_copy(
        src_ref=it_hbm.at[1],
        dst_ref=before,
        send_sem=prev_sem.at[0],
        recv_sem=prev_sem.at[1],
        device_id=right,
        device_id_type=MESH,
    )
    first = pltpu.make_async_copy(init_hbm, before, prev_sem.at[2])

    @pl.when(t < count - 1)
    def _():
        onward.start()

    @pl.when(t == 0)
    def _():
        first.start()

    rims = [
        pltpu.make_async_remote_copy(
            src_ref=di_hbm,
            dst_ref=d_ext.at[pl.ds(pl.multiple_of(16 + rows * c, 8), rows)],
            send_sem=rim_send.at[0],
            recv_sem=rim_recv.at[0],
            device_id=partner,
            device_id_type=MESH,
        ),
        pltpu.make_async_remote_copy(
            src_ref=it_hbm.at[:, pl.ds(pl.multiple_of((1 - c) * (rows - 8), 8), 8)],
            dst_ref=u_ext.at[:, pl.ds(pl.multiple_of(c * (rows + 8), 8), 8)],
            send_sem=rim_send.at[1],
            recv_sem=rim_recv.at[1],
            device_id=partner,
            device_id_type=MESH,
        ),
    ]
    for rim in rims:
        rim.start()

    for load in loads:
        load.wait()
    for rim in rims:
        rim.wait_recv()
    d_ext[0:16, :] = jnp.broadcast_to(d_ext[16:24, :][:1], (16, cols))
    last = 2 * rows + 16
    d_ext[last : last + 16, :] = jnp.broadcast_to(d_ext[last - 8 : last, :][7:8], (16, cols))

    def lane_of(shape):
        return lax.broadcasted_iota(jnp.int32, shape, 1)

    def residual(step, start):
        tall = slab + 16
        u = u_ext[step, pl.ds(start, tall), :]
        d = d_ext[pl.ds(pl.multiple_of(rows * c + start + 8, 8), tall), :]
        lane = lane_of((slab, cols))
        mid = slice(8, slab + 8)
        uc, dc = u[mid], d[mid]
        u_n, u_s = pltpu.roll(u, 1, 0)[mid], pltpu.roll(u, tall - 1, 0)[mid]
        d_n, d_s = pltpu.roll(d, 1, 0)[mid], pltpu.roll(d, tall - 1, 0)[mid]
        u_w = jnp.where(lane == 0, 0.0, pltpu.roll(uc, 1, 1))
        u_e = jnp.where(lane == cols - 1, 0.0, pltpu.roll(uc, cols - 1, 1))
        d_w = jnp.where(lane == 0, dc, pltpu.roll(dc, 1, 1))
        d_e = jnp.where(lane == cols - 1, dc, pltpu.roll(dc, cols - 1, 1))
        spread = (
            (dc + d_n) * (uc - u_n)
            + (dc + d_s) * (uc - u_s)
            + (dc + d_w) * (uc - u_w)
            + (dc + d_e) * (uc - u_e)
        )
        if step == 0:
            prev = before[pl.ds(start, slab), :]
        else:
            prev = u_ext[step - 1, pl.ds(pl.multiple_of(start + 8, 8), slab), :]
        value = time_step * force[step, pl.ds(start, slab), :] + prev - uc
        return value - (0.5 * time_step) * spread

    def squares(value):
        sq = value * value
        folded = sq[0:8]
        for i in range(1, slab // 8):
            folded = folded + sq[8 * i : 8 * i + 8]
        total_sq = folded[:, 0:128]
        for i in range(1, tiles):
            total_sq = total_sq + folded[:, 128 * i : 128 * i + 128]
        return total_sq

    def forward(step, dest, core):
        start = pl.multiple_of(lax.rem(dest, half) * slab + piece * core, 8)
        return pltpu.make_async_remote_copy(
            src_ref=res.at[step, pl.ds(start, piece)],
            dst_ref=by_cell.at[2 * t + step],
            send_sem=a_send.at[step, lax.rem(dest, half), core],
            recv_sem=a_recv.at[step, t],
            device_id={"tm": dest, "rows": core},
            device_id_type=MESH,
        )

    def chip(j):
        return half * c + lax.rem(t + half // 2 + j, half)

    def elsewhere(dest, core):
        return jnp.logical_or(dest != t, core != c)

    def peer(k):
        far = count // 2 - (k + 1) // 2
        return lax.rem(t + jnp.where(lax.rem(k, 2) == 1, far, count - far), count)

    def make(step, dest):
        start = pl.multiple_of(lax.rem(dest, half) * slab, slab)
        value = residual(step, start)
        res[step, pl.ds(start, slab), :] = value * tab[2 * t + step]
        sq_send[step] = sq_send[step] + squares(value)

    def send_one(step, dest):
        @pl.when(dest // half == c)
        def _():
            make(step, dest)
            forward(step, dest, 0).start()
            forward(step, dest, 1).start()

    def send_home(step):
        @pl.when(home == c)
        def _():
            make(step, t)
            start = pl.multiple_of(place * slab + piece * c, 8)
            by_cell[2 * t + step] = res[step, pl.ds(start, piece), :]
            forward(step, t, 1 - c).start()

    def widen(k, carry):
        pl.semaphore_signal(from_left, inc=1, device_id=right, device_id_type=MESH)
        pl.semaphore_signal(from_right, inc=1, device_id=left, device_id_type=MESH)
        pl.semaphore_wait(from_left, 1)
        pl.semaphore_wait(from_right, 1)
        send_one(1, lax.rem(t + k, count))

        @pl.when(k < half)
        def _():
            send_one(1, lax.rem(t + count - k, count))

        return carry

    sq_send[...] = jnp.zeros((2, 8, 128), jnp.float32)
    lax.fori_loop(1, half + 1, widen, 0)
    send_home(1)

    @pl.when(t > 0)
    def _():
        onward.wait_recv()

    @pl.when(t == 0)
    def _():
        first.wait()

    def send_far(k, carry):
        send_one(0, peer(k))
        return carry

    lax.fori_loop(0, count - 1, send_far, 0)
    send_home(0)

    sq_copy = pltpu.make_async_remote_copy(
        src_ref=sq_send,
        dst_ref=sq_recv,
        send_sem=rim_send.at[2],
        recv_sem=rim_recv.at[2],
        device_id=partner,
        device_id_type=MESH,
    )
    sq_copy.start()

    d = d_ext[pl.ds(pl.multiple_of(t * slab, slab), slab + 32), :]
    tall = slab + 16
    mid = slice(8, slab + 24)
    dc = d[mid]
    lane = lane_of((tall, cols))
    line = lax.broadcasted_iota(jnp.int32, (tall, cols), 0)
    outside = ((t == 0) & (line < 8)) | ((t == count - 1) & (line >= slab + 8))
    quarter = 0.5 * time_step
    w_n = quarter * (dc + pltpu.roll(d, 1, 0)[mid])
    w_s = quarter * (dc + pltpu.roll(d, slab + 31, 0)[mid])
    w_w = quarter * (dc + jnp.where(lane == 0, dc, pltpu.roll(dc, 1, 1)))
    w_e = quarter * (dc + jnp.where(lane == cols - 1, dc, pltpu.roll(dc, cols - 1, 1)))
    weights[0] = w_n + w_s + w_w + w_e
    weights[1] = jnp.where(outside, 0.0, w_n)
    weights[2] = jnp.where(outside, 0.0, w_s)
    weights[3] = jnp.where(lane == 0, 0.0, w_w)
    weights[4] = jnp.where(lane == cols - 1, 0.0, w_e)

    def arrival(step, source):
        return pltpu.make_async_remote_copy(
            src_ref=res.at[step, pl.ds(0, piece)],
            dst_ref=by_cell.at[2 * source + step],
            send_sem=a_send.at[step, 0, 0],
            recv_sem=a_recv.at[step, source],
            device_id={"tm": source},
            device_id_type=MESH,
        )

    def arrived(k, carry):
        for step in (0, 1):
            arrival(step, lax.rem(t + k, count)).wait_recv()
        return carry

    lax.fori_loop(1, count, arrived, 0)

    @pl.when(home != c)
    def _():
        for step in (0, 1):
            arrival(step, t).wait_recv()

    row_tiles = piece // 8

    def transform(p, carry):
        r = pl.multiple_of((p // tiles) * 8, 8)
        q = pl.multiple_of(lax.rem(p, tiles) * 128, 128)
        x = [by_cell[n, pl.ds(r, 8), pl.ds(q, 128)] for n in range(length)]
        f = rfft_list(x)
        here = (pl.ds(pl.multiple_of(r + 8 + piece * c, 8), 8), pl.ds(q, 128))
        spec[(0, 0) + here] = f[0][0]
        spec[(0, 1) + here] = f[pairs][0]
        for j in range(1, pairs):
            for part in (0, 1):
                spec[(j // share, 2 * (j % share) + part) + here] = f[j][part]
        return carry

    lax.fori_loop(0, row_tiles * tiles, transform, 0)

    beyond = {"tm": lax.rem(t + count + 2 * c - 1, count)}
    src_edge = pl.ds(pl.multiple_of(8 + (slab - 8) * c, 8), 8)
    dst_edge = pl.ds(pl.multiple_of((slab + 8) * (1 - c), 8), 8)

    def halo(group, q):
        fields = pl.ds(2 * q, 2)
        return pltpu.make_async_remote_copy(
            src_ref=spec.at[group, fields, src_edge],
            dst_ref=spec.at[group, fields, dst_edge],
            send_sem=h_send.at[group, q],
            recv_sem=h_recv.at[1 - c, q],
            device_id={**beyond, "rows": group},
            device_id_type=MESH,
        )

    own_part = pl.ds(pl.multiple_of(8 + piece * c, 8), piece)

    def swap(q):
        fields = pl.ds(2 * q, 2)
        return pltpu.make_async_remote_copy(
            src_ref=spec.at[1 - c, fields, own_part],
            dst_ref=spec.at[1 - c, fields, own_part],
            send_sem=x_send.at[q],
            recv_sem=x_recv.at[q],
            device_id=partner,
            device_id_type=MESH,
        )

    def send_halo(q, carry):
        halo(0, q).start()
        halo(1, q).start()
        swap(q).start()
        return carry

    lax.fori_loop(0, share, send_halo, 0)

    top = jnp.where(t == 0, 0.0, 1.0)
    bottom = jnp.where(t == count - 1, 0.0, 1.0)
    n_tr = slab // 8 + 2
    sub = lax.broadcasted_iota(jnp.int32, (8, cols), 0)

    def spread_of(v, wanted, shift):
        down = [pltpu.roll(x, 1, 0) for x in v]
        up = [pltpu.roll(x, 7, 0) for x in v]
        out = {}
        for i in wanted:
            v_n = jnp.where(sub == 0, down[max(i - 1, 0)], down[i])
            v_s = jnp.where(sub == 7, up[min(i + 1, n_tr - 1)], up[i])
            here = slice(8 * i, 8 * i + 8)
            out[i] = (
                (weights[0, here, :] + shift) * v[i]
                - weights[1, here, :] * v_n
                - weights[2, here, :] * v_s
                - weights[3, here, :] * pltpu.roll(v[i], 1, 1)
                - weights[4, here, :] * pltpu.roll(v[i], cols - 1, 1)
            )
        return out

    def clip(i, x):
        if i == 0:
            return x * top
        if i == n_tr - 1:
            return x * bottom
        return x

    inner = range(1, n_tr - 1)

    def folded(v):
        acc = None
        for i in inner:
            sq = v[i] * v[i]
            for k in range(tiles):
                part = sq[:, 128 * k : 128 * k + 128]
                acc = part if acc is None else acc + part
        return jnp.sum(acc, axis=0, keepdims=True)

    def solve(q, carry):
        for side in (0, 1):
            pltpu.make_async_remote_copy(
                src_ref=spec.at[c, pl.ds(2 * q, 2), src_edge],
                dst_ref=spec.at[c, pl.ds(2 * q, 2), pl.ds((slab + 8) * side, 8)],
                send_sem=h_send.at[0, q],
                recv_sem=h_recv.at[side, q],
                device_id=partner,
                device_id_type=MESH,
            ).wait_recv()
        pltpu.make_async_remote_copy(
            src_ref=spec.at[c, pl.ds(2 * q, 2), own_part],
            dst_ref=spec.at[c, pl.ds(2 * q, 2), pl.ds(pl.multiple_of(8 + piece * (1 - c), 8), piece)],
            send_sem=x_send.at[q],
            recv_sem=x_recv.at[q],
            device_id=partner,
            device_id_type=MESH,
        ).wait_recv()
        j = 2 * length + share * c + q
        a_re, a_im, b = tab[j], tab[j + pairs], tab[j + 2 * pairs]
        v = [
            [clip(i, spec[c, 2 * q + part, 8 * i : 8 * i + 8, :]) for i in range(n_tr)]
            for part in (0, 1)
        ]
        for order in range(6):
            wanted = inner if order == 5 else range(n_tr)
            sign = b if order % 2 == 0 else -b
            k_re, k_im = spread_of(v[0], wanted, a_re), spread_of(v[1], wanted, a_im)
            new_re, new_im = [None] * n_tr, [None] * n_tr
            for i in wanted:
                new_re[i] = sign * v[1][i] + k_re[i]
                new_im[i] = k_im[i] - sign * v[0][i]
            v = [new_re, new_im]
            mom[2 * order, pl.ds(q, 1), :] = folded(v[0])
            mom[2 * order + 1, pl.ds(q, 1), :] = folded(v[1])
            if order % 2 == 0:
                keep = (v0_ref, v1_ref, v2_ref)[order // 2]
                for part in (0, 1):
                    for i in inner:
                        keep[2 * q + part, 8 * i - 8 : 8 * i, :] = v[part][i]
        return carry

    lax.fori_loop(0, share, solve, 0)

    lane8 = lax.broadcasted_iota(jnp.int32, (8, 128), 1)
    row8 = lax.broadcasted_iota(jnp.int32, (8, 128), 0)
    apart = (row8 == 0) & (c == 0)
    packed = [jnp.zeros((8, 128), jnp.float32), jnp.zeros((8, 128), jnp.float32)]

    def slot(k, g):
        return lane8 == (16 * row8 + k if g == 0 else 16 * k + 12)

    for k in range(6):
        re, im = mom[2 * k], mom[2 * k + 1]
        both = jnp.where(apart, re, re + im)
        for g, x in enumerate((both, im)):
            big = 256.0 * jnp.max(x, axis=1, keepdims=True)
            hi = (x + big) - big
            lo = x - hi
            where = slot(k, g) if g == 0 else slot(k, g) & (row8 == 0)
            packed[0] = jnp.where(where, jnp.sum(hi, axis=1, keepdims=True), packed[0])
            packed[1] = jnp.where(where, jnp.sum(lo, axis=1, keepdims=True), packed[1])
    mine = jnp.concatenate([jnp.sum(x, axis=0, keepdims=True) for x in packed], axis=1)
    ar_send[...] = mine
    ar_all[t] = mine

    def tell(k):
        return pltpu.make_async_remote_copy(
            src_ref=ar_send,
            dst_ref=ar_all.at[t],
            send_sem=m_send.at[k],
            recv_sem=m_recv.at[t],
            device_id={"tm": lax.rem(t + k, count)},
            device_id_type=MESH,
        )

    def tell_one(k, carry):
        tell(k).start()
        return carry

    lax.fori_loop(1, count, tell_one, 0)

    def told(k, carry):
        source = lax.rem(t + k, count)
        pltpu.make_async_remote_copy(
            src_ref=ar_send,
            dst_ref=ar_all.at[source],
            send_sem=m_send.at[k],
            recv_sem=m_recv.at[source],
            device_id={"tm": source},
            device_id_type=MESH,
        ).wait_recv()
        return carry

    lax.fori_loop(1, count, told, 0)
    sums = [(ar_all[i][:, 0:128], ar_all[i][:, 128:256]) for i in range(count)]
    while len(sums) > 1:
        sums = [pair_add(sums[2 * i], sums[2 * i + 1]) for i in range(len(sums) // 2)]
    whole = [jnp.broadcast_to(x, (8, 128)) for x in sums[0]]
    mu = []
    for k in range(6):
        sides = []
        for x in whole:
            groups = [
                jnp.broadcast_to(
                    jnp.sum(jnp.where(slot(k, g), x, 0.0), axis=1, keepdims=True), (8, 128)
                )
                for g in range(2)
            ]
            sides.append(jnp.concatenate(groups, axis=0))
        mu.append(tuple(sides))
    for k, w in enumerate(krylov_weights(mu)):
        coef[k, 0] = w[0:share]
        coef[k, 1] = jnp.where(apart, w[share : share + 1], w[0:share])

    def blend(q, part_rows):
        for part in (0, 1):
            f = 2 * q + part
            total = None
            for k, ref in enumerate((v0_ref, v1_ref, v2_ref)):
                w = jnp.concatenate([coef[k, part, pl.ds(q, 1), :]] * tiles, axis=1)
                term = w * ref[f, part_rows, :]
                total = term if total is None else total + term
            xs[c, f, part_rows, :] = total

    my_rows = pl.ds(pl.multiple_of(piece * c, piece), piece)
    other_rows = pl.ds(pl.multiple_of(piece * (1 - c), piece), piece)

    def give(q, part_rows, group):
        block = xs.at[group, pl.ds(2 * q, 2), part_rows]
        return pltpu.make_async_remote_copy(
            src_ref=block,
            dst_ref=block,
            send_sem=y_send.at[q],
            recv_sem=y_recv.at[q],
            device_id=partner,
            device_id_type=MESH,
        )

    def blend_other(q, carry):
        blend(q, other_rows)
        give(q, other_rows, c).start()
        return carry

    lax.fori_loop(0, share, blend_other, 0)

    def blend_own(q, carry):
        blend(q, my_rows)
        return carry

    lax.fori_loop(0, share, blend_own, 0)

    def given(q, carry):
        give(q, my_rows, 1 - c).wait_recv()
        return carry

    lax.fori_loop(0, share, given, 0)

    def restore(p, carry):
        r = pl.multiple_of((p // tiles) * 8, 8)
        q = pl.multiple_of(lax.rem(p, tiles) * 128, 128)
        here = (pl.ds(pl.multiple_of(r + piece * c, 8), 8), pl.ds(q, 128))
        freq = [(xs[(0, 0) + here], None)]
        for j in range(1, pairs):
            freq.append(tuple(xs[(j // share, 2 * (j % share) + part) + here] for part in (0, 1)))
        freq.append((xs[(0, 1) + here], None))
        for n, x in enumerate(irfft_list(freq)):
            corr[n, pl.ds(r, 8), pl.ds(q, 128)] = x * tab[length + n]
        return carry

    lax.fori_loop(0, row_tiles * tiles, restore, 0)

    def block_of(source, core):
        return pl.multiple_of(lax.rem(source, half) * slab + piece * core, 8)

    def returning(dest):
        return pltpu.make_async_remote_copy(
            src_ref=corr.at[pl.ds(2 * dest, 2)],
            dst_ref=back.at[:, pl.ds(block_of(t, c), piece)],
            send_sem=b_send.at[dest],
            recv_sem=b_recv.at[place, c],
            device_id={"tm": dest, "rows": home},
            device_id_type=MESH,
        )

    def send_back(k, carry):
        returning(peer(k)).start()
        return carry

    lax.fori_loop(0, count - 1, send_back, 0)

    @pl.when(home != c)
    def _():
        returning(t).start()

    sq_copy.wait()
    rms = jnp.sqrt(
        jnp.sum(jnp.sum(sq_send[...] + sq_recv[...], axis=2, keepdims=True), axis=1, keepdims=True) / cells
        + rms_eps
    )
    rms_ref[...] = jnp.broadcast_to(rms[:, 0], (2, 128))

    def final(source, core, piece_of):
        start = block_of(source, core)
        ahead = pl.ds(pl.multiple_of(start + 8, 8), piece)
        out_ref[:, pl.ds(start, piece), :] = u_ext[:, ahead, :] + piece_of

    @pl.when(home == c)
    def _():
        final(t, c, corr[pl.ds(2 * t, 2)])

    def returned(j, carry):
        source = chip(j)
        for core in (0, 1):

            @pl.when(elsewhere(source, core))
            def _():
                block = pl.ds(block_of(source, core), piece)
                pltpu.make_async_remote_copy(
                    src_ref=corr.at[pl.ds(0, 2)],
                    dst_ref=back.at[:, block],
                    send_sem=b_send.at[0],
                    recv_sem=b_recv.at[lax.rem(source, half), core],
                    device_id={"tm": source},
                    device_id_type=MESH,
                ).wait_recv()
                final(source, core, back[:, block, :])

        return carry

    lax.fori_loop(0, half, returned, 0)

    for rim in rims:
        rim.wait_send()

    @pl.when(t < count - 1)
    def _():
        onward.wait_send()

    def drain_forward(j, carry):
        dest = chip(j)
        for core in (0, 1):

            @pl.when(elsewhere(dest, core))
            def _():
                forward(0, dest, core).wait_send()
                forward(1, dest, core).wait_send()

        return carry

    lax.fori_loop(0, half, drain_forward, 0)

    def drain_back(k, carry):
        returning(peer(k)).wait_send()
        return carry

    lax.fori_loop(0, count - 1, drain_back, 0)

    @pl.when(home != c)
    def _():
        returning(t).wait_send()

    def drain_pairs(q, carry):
        halo(0, q).wait_send()
        halo(1, q).wait_send()
        swap(q).wait_send()
        give(q, other_rows, c).wait_send()
        return carry

    lax.fori_loop(0, share, drain_pairs, 0)

    def drain_tell(k, carry):
        tell(k).wait_send()
        return carry

    lax.fori_loop(1, count, drain_tell, 0)


def tables(length):
    pairs = length // 2
    n = np.arange(length)
    growth = np.exp(np.log(circulant_alpha) * n / length)
    root = np.exp(np.log(circulant_alpha) / length)
    j = np.arange(pairs)
    a_re = 1.0 - root * np.cos(2.0 * np.pi * j / length)
    a_im = a_re.copy()
    a_im[0] = 1.0 + root
    b = root * np.sin(2.0 * np.pi * j / length)
    return np.concatenate([growth, 1.0 / (length * growth), a_re, a_im, b]).astype(np.float32)


def shards(iterate, forcing, initial_state, diffusivity):
    steps, rows, cols = iterate.shape
    count = lax.axis_size("tm")
    halves = lax.axis_size("rows")
    length = steps * count
    assert steps == 2 and halves == 2
    slab = 2 * rows // count
    pairs = length // 2
    share = pairs // 2
    cells = rows * halves * cols
    f32 = jnp.float32
    vmem = pltpu.VMEM
    dma = pltpu.SemaphoreType.DMA
    hbm = pl.BlockSpec(memory_space=pl.ANY)
    updated, rms = pl.pallas_call(
        functools.partial(kernel, count, cells),
        out_shape=(
            vmem((steps, rows, cols), f32),
            vmem((steps, 128), f32),
        ),
        in_specs=[hbm] * 4 + [pl.BlockSpec(memory_space=pltpu.SMEM)],
        out_specs=(pl.BlockSpec(memory_space=vmem), pl.BlockSpec(memory_space=vmem)),
        scratch_shapes=[
            vmem((steps, rows + 16, cols), f32),
            vmem((steps, rows, cols), f32),
            vmem((rows, cols), f32),
            vmem((2 * rows + 32, cols), f32),
            vmem((steps, rows, cols), f32),
            vmem((length, slab // 2, cols), f32),
            vmem((2, pairs, slab + 16, cols), f32),
            vmem((pairs, slab, cols), f32),
            vmem((pairs, slab, cols), f32),
            vmem((pairs, slab, cols), f32),
            vmem((2, pairs, slab, cols), f32),
            vmem((length, slab // 2, cols), f32),
            vmem((steps, rows, cols), f32),
            vmem((5, slab + 16, cols), f32),
            vmem((12, share, 128), f32),
            vmem((3, 2, share, 128), f32),
            vmem((1, 256), f32),
            vmem((count, 1, 256), f32),
            vmem((2, 8, 128), f32),
            vmem((2, 8, 128), f32),
            dma((3,)),
            dma((3,)),
            dma((3,)),
            dma((3,)),
            dma((2, count // 2, 2)),
            dma((2, count)),
            dma((2, share)),
            dma((2, share)),
            dma((share,)),
            dma((share,)),
            dma((share,)),
            dma((share,)),
            dma((count,)),
            dma((count,)),
            dma((count,)),
            dma((count // 2, 2)),
            pltpu.SemaphoreType.REGULAR,
            pltpu.SemaphoreType.REGULAR,
        ],
        compiler_params=pltpu.CompilerParams(collective_id=0, has_side_effects=True),
        name="paradiag",
    )(iterate, forcing, initial_state, diffusivity, jnp.asarray(tables(length)))
    return updated, rms[:, 0]


def solution(mesh):
    placed = (
        P(("groups", "tm"), "rows", None),
        P(("groups", "tm"), "rows", None),
        P(("groups", "rows"), None),
        P(("groups", "rows"), None),
    )
    return jax.shard_map(
        shards,
        mesh=mesh,
        in_specs=placed,
        out_specs=(P(("groups", "tm"), "rows", None), P(("groups", "tm"))),
        check_vma=False,
    )
```

```python
import functools

import jax
import jax.numpy as jnp
import numpy as np
from jax import lax
from jax.experimental import pallas as pl
from jax.experimental.pallas import tpu as pltpu
from jax.sharding import PartitionSpec as P

circulant_alpha = 0.05
time_step = 0.5
rms_eps = 1e-06
MESH = pl.DeviceIdType.MESH


def rfft_list(x):
    n = len(x)
    if n == 1:
        return [(x[0], None)]
    even, odd = rfft_list(x[0::2]), rfft_list(x[1::2])
    half = n // 2
    out = [None] * (half + 1)
    out[0] = (even[0][0] + odd[0][0], None)
    out[half] = (even[0][0] - odd[0][0], None)
    for k in range(1, half // 2 + 1):
        if 2 * k == half:
            out[k] = (even[k][0], -odd[k][0])
            continue
        angle = 2.0 * np.pi * k / n
        cos, sin = float(np.cos(angle)), float(np.sin(angle))
        o_re, o_im = odd[k]
        if 8 * k == n:
            t_re, t_im = (o_re + o_im) * cos, (o_im - o_re) * cos
        else:
            t_re, t_im = o_re * cos + o_im * sin, o_im * cos - o_re * sin
        e_re, e_im = even[k]
        out[k] = (e_re + t_re, e_im + t_im)
        out[half - k] = (e_re - t_re, t_im - e_im)
    return out


def irfft_list(freq):
    half = len(freq) - 1
    n = 2 * half
    if n == 2:
        return [freq[0][0] + freq[1][0], freq[0][0] - freq[1][0]]
    even, odd = [None] * (half // 2 + 1), [None] * (half // 2 + 1)
    even[0] = (freq[0][0] + freq[half][0], None)
    odd[0] = (freq[0][0] - freq[half][0], None)
    for k in range(1, half // 2 + 1):
        if 2 * k == half:
            even[k] = (freq[k][0] + freq[k][0], None)
            odd[k] = (-(freq[k][1] + freq[k][1]), None)
            continue
        angle = 2.0 * np.pi * k / n
        cos, sin = float(np.cos(angle)), float(np.sin(angle))
        a_re, a_im = freq[k]
        b_re, b_im = freq[half - k]
        even[k] = (a_re + b_re, a_im - b_im)
        d_re, d_im = a_re - b_re, a_im + b_im
        if 8 * k == n:
            odd[k] = ((d_re - d_im) * cos, (d_re + d_im) * cos)
        else:
            odd[k] = (d_re * cos - d_im * sin, d_im * cos + d_re * sin)
    even_out, odd_out = irfft_list(even), irfft_list(odd)
    out = [None] * n
    out[0::2], out[1::2] = even_out, odd_out
    return out


def two_sum(a, b):
    s = a + b
    v = s - a
    return s, (a - (s - v)) + (b - v)


def quick_sum(a, b):
    s = a + b
    return s, b - (s - a)


def split(a):
    t = 4097.0 * a
    hi = t - (t - a)
    return hi, a - hi


def two_prod(a, b):
    p = a * b
    ah, al = split(a)
    bh, bl = split(b)
    return p, ((ah * bh - p) + ah * bl + al * bh) + al * bl


def pair_add(x, y):
    s, e = two_sum(x[0], y[0])
    return quick_sum(s, e + (x[1] + y[1]))


def pair_neg(x):
    return (-x[0], -x[1])


def pair_mul(x, y):
    p, e = two_prod(x[0], y[0])
    return quick_sum(p, e + (x[0] * y[1] + x[1] * y[0]))


def pair_div(x, y):
    q = x[0] / y[0]
    rest = pair_add(x, pair_neg(pair_mul((q, jnp.zeros_like(q)), y)))
    return quick_sum(q, rest[0] / y[0])


def krylov_weights(mu):
    one = (jnp.ones_like(mu[0][0]), jnp.zeros_like(mu[0][0]))
    zero = jnp.zeros_like(mu[0][0])
    inv0 = pair_div(one, mu[0])
    t1 = pair_div(mu[0], mu[1])
    t2 = pair_mul(t1, t1)
    t3 = pair_mul(t2, t1)
    t4 = pair_mul(t2, t2)
    t5 = pair_mul(t4, t1)
    m2, m3, m4, m5 = (
        pair_mul(pair_mul(mu[k], inv0), t) for k, t in ((2, t2), (3, t3), (4, t4), (5, t5))
    )
    tiny = 2.0**-32
    gain0 = pair_add(m2, pair_neg(one))
    den1 = pair_add(m3, pair_neg(pair_mul(m2, m2)))
    ok1 = (gain0[0] > tiny) & (den1[0] > tiny * m3[0])

    def kept(ok, x, other):
        return (jnp.where(ok, x[0], other), jnp.where(ok, x[1], 0.0))

    rate1 = kept(ok1, pair_div(kept(ok1, gain0, 0.0), kept(ok1, den1, 1.0)), 0.0)
    mid = pair_add(one, pair_mul(rate1, m2))
    inner = pair_add(pair_add(m2, pair_neg(pair_mul(mid, m3))), pair_mul(rate1, m4))
    size = m2[0] + mid[0] * m3[0] + rate1[0] * m4[0]
    ok2 = ok1 & (inner[0] > tiny * size)
    gamma2 = pair_mul(rate1, kept(ok2, inner, 0.0))
    gain1 = pair_div(gamma2, kept(ok1, gain0, 1.0))
    base = pair_add(one, pair_mul(gain1, m2))
    slope = pair_add(mid, gain1)
    inner2 = pair_add(
        pair_add(pair_mul(base, m3), pair_neg(pair_mul(slope, m4))), pair_mul(rate1, m5)
    )
    size2 = base[0] * m3[0] + slope[0] * m4[0] + rate1[0] * m5[0]
    ok3 = ok2 & (inner2[0] > tiny * size2)
    ratio = kept(ok2, inner, 0.0)
    rate2 = pair_div(ratio, kept(ok3, inner2, 1.0))
    rate2 = jnp.where(ok3, rate2[0], zero)
    w0 = mid[0] + rate2 * base[0]
    w1 = -(rate1[0] + rate2 * slope[0])
    w2 = rate2 * rate1[0]
    return w0 * t1[0], w1 * t2[0], w2 * t3[0]


def kernel(
    count,
    cells,
    it_hbm,
    fo_hbm,
    init_hbm,
    di_hbm,
    tab,
    out_ref,
    rms_ref,
    u_ext,
    force,
    before,
    d_ext,
    res,
    by_cell,
    stop,
    spec,
    basis,
    corr,
    back,
    weights,
    lined,
    mom,
    coef,
    ar_send,
    ar_all,
    sq_send,
    sq_recv,
    load_sem,
    prev_sem,
    hop_sem,
    rim_send,
    rim_recv,
    a_send,
    a_recv,
    h_send,
    h_recv,
    x_send,
    x_recv,
    y_send,
    y_recv,
    m_send,
    m_recv,
    b_send,
    b_recv,
    from_left,
    from_right,
):
    t = lax.axis_index("tm")
    c = lax.axis_index("rows")
    me = c * count + t
    total = 2 * count
    length = 2 * count
    pairs = length // 2
    share = pairs // 2
    rows = force.shape[1]
    cols = force.shape[2]
    half = count // 2
    slab = rows // half
    piece = slab // 2
    tiles = cols // 128
    home = t // half
    place = lax.rem(t, half)

    def pos(i):
        return {"tm": lax.rem(i, count), "rows": i // count}

    barrier = pltpu.get_barrier_semaphore()

    right, left = {"tm": lax.rem(t + 1, count)}, {"tm": lax.rem(t + count - 1, count)}
    partner = {"rows": 1 - c}
    for neighbour in (left, right, partner):
        pl.semaphore_signal(barrier, inc=1, device_id=neighbour, device_id_type=MESH)

    loads = [
        pltpu.make_async_copy(di_hbm, d_ext.at[pl.ds(pl.multiple_of(16 + rows * c, 8), rows)], load_sem.at[0]),
        pltpu.make_async_copy(it_hbm, u_ext.at[:, pl.ds(8, rows)], load_sem.at[1]),
        pltpu.make_async_copy(fo_hbm, force, load_sem.at[2]),
    ]
    for load in loads:
        load.start()
    u_ext[:, pl.ds(pl.multiple_of(c * (rows + 8), 8), 8), :] = jnp.zeros((2, 8, cols), jnp.float32)
    pl.semaphore_wait(barrier, 3)

    onward = pltpu.make_async_remote_copy(
        src_ref=it_hbm.at[1],
        dst_ref=before,
        send_sem=prev_sem.at[0],
        recv_sem=prev_sem.at[1],
        device_id=right,
        device_id_type=MESH,
    )
    first = pltpu.make_async_copy(init_hbm, before, prev_sem.at[2])

    @pl.when(t < count - 1)
    def _():
        onward.start()

    @pl.when(t == 0)
    def _():
        first.start()

    rims = [
        pltpu.make_async_remote_copy(
            src_ref=di_hbm,
            dst_ref=d_ext.at[pl.ds(pl.multiple_of(16 + rows * c, 8), rows)],
            send_sem=rim_send.at[0],
            recv_sem=rim_recv.at[0],
            device_id=partner,
            device_id_type=MESH,
        ),
        pltpu.make_async_remote_copy(
            src_ref=it_hbm.at[:, pl.ds(pl.multiple_of((1 - c) * (rows - 8), 8), 8)],
            dst_ref=u_ext.at[:, pl.ds(pl.multiple_of(c * (rows + 8), 8), 8)],
            send_sem=rim_send.at[1],
            recv_sem=rim_recv.at[1],
            device_id=partner,
            device_id_type=MESH,
        ),
    ]
    for rim in rims:
        rim.start()

    for load in loads:
        load.wait()
    for rim in rims:
        rim.wait_recv()
    d_ext[0:16, :] = jnp.broadcast_to(d_ext[16:24, :][:1], (16, cols))
    last = 2 * rows + 16
    d_ext[last : last + 16, :] = jnp.broadcast_to(d_ext[last - 8 : last, :][7:8], (16, cols))

    def lane_of(shape):
        return lax.broadcasted_iota(jnp.int32, shape, 1)

    def residual(step, start):
        tall = slab + 16
        u = u_ext[step, pl.ds(start, tall), :]
        d = d_ext[pl.ds(pl.multiple_of(rows * c + start + 8, 8), tall), :]
        lane = lane_of((slab, cols))
        mid = slice(8, slab + 8)
        uc, dc = u[mid], d[mid]
        u_n, u_s = pltpu.roll(u, 1, 0)[mid], pltpu.roll(u, tall - 1, 0)[mid]
        d_n, d_s = pltpu.roll(d, 1, 0)[mid], pltpu.roll(d, tall - 1, 0)[mid]
        u_w = jnp.where(lane == 0, 0.0, pltpu.roll(uc, 1, 1))
        u_e = jnp.where(lane == cols - 1, 0.0, pltpu.roll(uc, cols - 1, 1))
        d_w = jnp.where(lane == 0, dc, pltpu.roll(dc, 1, 1))
        d_e = jnp.where(lane == cols - 1, dc, pltpu.roll(dc, cols - 1, 1))
        spread = (
            (dc + d_n) * (uc - u_n)
            + (dc + d_s) * (uc - u_s)
            + (dc + d_w) * (uc - u_w)
            + (dc + d_e) * (uc - u_e)
        )
        if step == 0:
            prev = before[pl.ds(start, slab), :]
        else:
            prev = u_ext[step - 1, pl.ds(pl.multiple_of(start + 8, 8), slab), :]
        value = time_step * force[step, pl.ds(start, slab), :] + prev - uc
        return value - (0.5 * time_step) * spread

    def squares(value):
        sq = value * value
        folded = sq[0:8]
        for i in range(1, slab // 8):
            folded = folded + sq[8 * i : 8 * i + 8]
        total_sq = folded[:, 0:128]
        for i in range(1, tiles):
            total_sq = total_sq + folded[:, 128 * i : 128 * i + 128]
        return total_sq

    def forward(step, dest, core):
        start = pl.multiple_of(lax.rem(dest, half) * slab + piece * core, 8)
        return pltpu.make_async_remote_copy(
            src_ref=res.at[step, pl.ds(start, piece)],
            dst_ref=by_cell.at[2 * t + step],
            send_sem=a_send.at[step, lax.rem(dest, half), core],
            recv_sem=a_recv.at[step, t],
            device_id={"tm": dest, "rows": core},
            device_id_type=MESH,
        )

    def chip(j):
        return half * c + lax.rem(t + half // 2 + j, half)

    def elsewhere(dest, core):
        return jnp.logical_or(dest != t, core != c)

    def peer(k):
        far = count // 2 - (k + 1) // 2
        return lax.rem(t + jnp.where(lax.rem(k, 2) == 1, far, count - far), count)

    def make(step, dest):
        start = pl.multiple_of(lax.rem(dest, half) * slab, slab)
        value = residual(step, start)
        res[step, pl.ds(start, slab), :] = value * tab[2 * t + step]
        sq_send[step] = sq_send[step] + squares(value)

    def send_one(step, dest):
        @pl.when(dest // half == c)
        def _():
            make(step, dest)
            forward(step, dest, 0).start()
            forward(step, dest, 1).start()

    def send_home(step):
        @pl.when(home == c)
        def _():
            make(step, t)
            start = pl.multiple_of(place * slab + piece * c, 8)
            by_cell[2 * t + step] = res[step, pl.ds(start, piece), :]
            forward(step, t, 1 - c).start()

    across = lax.rem(t + half, count)
    hop = pltpu.make_async_remote_copy(
        src_ref=res.at[1, pl.ds(pl.multiple_of(lax.rem(across, half) * slab, slab), slab)],
        dst_ref=stop,
        send_sem=hop_sem.at[0],
        recv_sem=hop_sem.at[1],
        device_id={"tm": lax.rem(t + count - half // 2, count)},
        device_id_type=MESH,
    )
    origin = lax.rem(t + half // 2, count)
    relays = lax.rem(origin + half, count) // half == c

    def hop_on(core):
        return pltpu.make_async_remote_copy(
            src_ref=stop.at[pl.ds(piece * core, piece)],
            dst_ref=by_cell.at[2 * origin + 1],
            send_sem=hop_sem.at[2 + core],
            recv_sem=a_recv.at[1, origin],
            device_id={"tm": lax.rem(t + count - half // 2, count), "rows": core},
            device_id_type=MESH,
        )

    def widen(k, carry):
        pl.semaphore_signal(from_left, inc=1, device_id=right, device_id_type=MESH)
        pl.semaphore_signal(from_right, inc=1, device_id=left, device_id_type=MESH)
        pl.semaphore_wait(from_left, 1)
        pl.semaphore_wait(from_right, 1)
        @pl.when(k < half)
        def _():
            send_one(1, lax.rem(t + k, count))
            send_one(1, lax.rem(t + count - k, count))

        @pl.when((k == half // 2) & (home != c))
        def _():
            make(1, across)
            hop.start()

        return carry

    sq_send[...] = jnp.zeros((2, 8, 128), jnp.float32)
    lax.fori_loop(1, half + 1, widen, 0)
    send_home(1)

    @pl.when(relays)
    def _():
        hop.wait_recv()
        hop_on(0).start()
        hop_on(1).start()

    @pl.when(t > 0)
    def _():
        onward.wait_recv()

    @pl.when(t == 0)
    def _():
        first.wait()

    def send_far(k, carry):
        send_one(0, peer(k))
        return carry

    lax.fori_loop(0, count - 1, send_far, 0)
    send_home(0)

    sq_copy = pltpu.make_async_remote_copy(
        src_ref=sq_send,
        dst_ref=sq_recv,
        send_sem=rim_send.at[2],
        recv_sem=rim_recv.at[2],
        device_id=partner,
        device_id_type=MESH,
    )
    sq_copy.start()

    d = d_ext[pl.ds(pl.multiple_of(t * slab, slab), slab + 32), :]
    tall = slab + 16
    mid = slice(8, slab + 24)
    dc = d[mid]
    lane = lane_of((tall, cols))
    line = lax.broadcasted_iota(jnp.int32, (tall, cols), 0)
    outside = ((t == 0) & (line < 8)) | ((t == count - 1) & (line >= slab + 8))
    quarter = 0.5 * time_step
    w_n = quarter * (dc + pltpu.roll(d, 1, 0)[mid])
    w_s = quarter * (dc + pltpu.roll(d, slab + 31, 0)[mid])
    w_w = quarter * (dc + jnp.where(lane == 0, dc, pltpu.roll(dc, 1, 1)))
    w_e = quarter * (dc + jnp.where(lane == cols - 1, dc, pltpu.roll(dc, cols - 1, 1)))
    weights[0] = w_n + w_s + w_w + w_e
    weights[1] = jnp.where(outside, 0.0, w_n)
    weights[2] = jnp.where(outside, 0.0, w_s)
    weights[3] = jnp.where(lane == 0, 0.0, w_w)
    weights[4] = jnp.where(lane == cols - 1, 0.0, w_e)

    def arrival(step, source):
        return pltpu.make_async_remote_copy(
            src_ref=res.at[step, pl.ds(0, piece)],
            dst_ref=by_cell.at[2 * source + step],
            send_sem=a_send.at[step, 0, 0],
            recv_sem=a_recv.at[step, source],
            device_id={"tm": source},
            device_id_type=MESH,
        )

    def arrived(k, carry):
        for step in (0, 1):
            arrival(step, lax.rem(t + k, count)).wait_recv()
        return carry

    lax.fori_loop(1, count, arrived, 0)

    @pl.when(home != c)
    def _():
        for step in (0, 1):
            arrival(step, t).wait_recv()

    row_tiles = piece // 8

    def transform(p, carry):
        r = pl.multiple_of((p // tiles) * 8, 8)
        q = pl.multiple_of(lax.rem(p, tiles) * 128, 128)
        x = [by_cell[n, pl.ds(r, 8), pl.ds(q, 128)] for n in range(length)]
        f = rfft_list(x)
        here = (pl.ds(pl.multiple_of(r + 8 + piece * c, 8), 8), pl.ds(q, 128))
        spec[(0, 0) + here] = f[0][0]
        spec[(0, 1) + here] = f[pairs][0]
        for j in range(1, pairs):
            for part in (0, 1):
                spec[(j // share, 2 * (j % share) + part) + here] = f[j][part]
        return carry

    lax.fori_loop(0, row_tiles * tiles, transform, 0)

    beyond = {"tm": lax.rem(t + count + 2 * c - 1, count)}
    src_edge = pl.ds(pl.multiple_of(8 + (slab - 8) * c, 8), 8)
    dst_edge = pl.ds(pl.multiple_of((slab + 8) * (1 - c), 8), 8)

    def halo(group, q):
        fields = pl.ds(2 * q, 2)
        return pltpu.make_async_remote_copy(
            src_ref=spec.at[group, fields, src_edge],
            dst_ref=spec.at[group, fields, dst_edge],
            send_sem=h_send.at[group, q],
            recv_sem=h_recv.at[1 - c, q],
            device_id={**beyond, "rows": group},
            device_id_type=MESH,
        )

    own_part = pl.ds(pl.multiple_of(8 + piece * c, 8), piece)

    def swap(q):
        fields = pl.ds(2 * q, 2)
        return pltpu.make_async_remote_copy(
            src_ref=spec.at[1 - c, fields, own_part],
            dst_ref=spec.at[1 - c, fields, own_part],
            send_sem=x_send.at[q],
            recv_sem=x_recv.at[q],
            device_id=partner,
            device_id_type=MESH,
        )

    def send_halo(q, carry):
        halo(0, q).start()
        halo(1, q).start()
        swap(q).start()
        return carry

    lax.fori_loop(0, share, send_halo, 0)

    top = jnp.where(t == 0, 0.0, 1.0)
    bottom = jnp.where(t == count - 1, 0.0, 1.0)
    n_tr = slab // 8 + 2

    def spread_of(v, wanted, shift, part):
        for i in range(n_tr):
            for k in range(tiles):
                lined[part, k, 8 * i + 8 : 8 * i + 16, :] = v[i][:, 128 * k : 128 * k + 128]
        out = {}
        for i in wanted:
            v_n, v_s = (
                jnp.concatenate(
                    [lined[part, k, 8 * i + 8 + o : 8 * i + 16 + o, :] for k in range(tiles)], axis=1
                )
                for o in (-1, 1)
            )
            here = slice(8 * i, 8 * i + 8)
            out[i] = (
                (weights[0, here, :] + shift) * v[i]
                - weights[1, here, :] * v_n
                - weights[2, here, :] * v_s
                - weights[3, here, :] * pltpu.roll(v[i], 1, 1)
                - weights[4, here, :] * pltpu.roll(v[i], cols - 1, 1)
            )
        return out

    def clip(i, x):
        if i == 0:
            return x * top
        if i == n_tr - 1:
            return x * bottom
        return x

    inner = range(1, n_tr - 1)

    def folded(v):
        acc = None
        for i in inner:
            sq = v[i] * v[i]
            for k in range(tiles):
                part = sq[:, 128 * k : 128 * k + 128]
                acc = part if acc is None else acc + part
        return jnp.sum(acc, axis=0, keepdims=True)

    def give(q):
        return pltpu.make_async_remote_copy(
            src_ref=basis.at[2, :, pl.ds(2 * q, 2)],
            dst_ref=basis.at[c, :, pl.ds(2 * q, 2)],
            send_sem=y_send.at[q],
            recv_sem=y_recv.at[q],
            device_id=partner,
            device_id_type=MESH,
        )

    def solve(q, carry):
        for side in (0, 1):
            pltpu.make_async_remote_copy(
                src_ref=spec.at[c, pl.ds(2 * q, 2), src_edge],
                dst_ref=spec.at[c, pl.ds(2 * q, 2), pl.ds((slab + 8) * side, 8)],
                send_sem=h_send.at[0, q],
                recv_sem=h_recv.at[side, q],
                device_id=partner,
                device_id_type=MESH,
            ).wait_recv()
        pltpu.make_async_remote_copy(
            src_ref=spec.at[c, pl.ds(2 * q, 2), own_part],
            dst_ref=spec.at[c, pl.ds(2 * q, 2), pl.ds(pl.multiple_of(8 + piece * (1 - c), 8), piece)],
            send_sem=x_send.at[q],
            recv_sem=x_recv.at[q],
            device_id=partner,
            device_id_type=MESH,
        ).wait_recv()
        j = 2 * length + share * c + q
        a_re, a_im, b = tab[j], tab[j + pairs], tab[j + 2 * pairs]
        v = [
            [clip(i, spec[c, 2 * q + part, 8 * i : 8 * i + 8, :]) for i in range(n_tr)]
            for part in (0, 1)
        ]
        for order in range(6):
            wanted = inner if order == 5 else range(n_tr)
            sign = b if order % 2 == 0 else -b
            k_re, k_im = spread_of(v[0], wanted, a_re, 0), spread_of(v[1], wanted, a_im, 1)
            new_re, new_im = [None] * n_tr, [None] * n_tr
            for i in wanted:
                new_re[i] = sign * v[1][i] + k_re[i]
                new_im[i] = k_im[i] - sign * v[0][i]
            v = [new_re, new_im]
            mom[2 * order, pl.ds(q, 1), :] = folded(v[0])
            mom[2 * order + 1, pl.ds(q, 1), :] = folded(v[1])
            if order % 2 == 0:
                for part in (0, 1):
                    for i in inner:
                        line = (8 * i - 8) % piece
                        keep = 2 * c if 8 * i - 8 < piece else 2 - c
                        basis[keep, order // 2, 2 * q + part, line : line + 8, :] = v[part][i]
        give(q).start()
        return carry

    lined[...] = jnp.zeros(lined.shape, jnp.float32)
    lax.fori_loop(0, share, solve, 0)

    lane8 = lax.broadcasted_iota(jnp.int32, (8, 128), 1)
    row8 = lax.broadcasted_iota(jnp.int32, (8, 128), 0)
    row16 = lax.broadcasted_iota(jnp.int32, (pairs, 128), 0)
    apart = (row8 == 0) & (c == 0)
    packed = [jnp.zeros((8, 128), jnp.float32), jnp.zeros((8, 128), jnp.float32)]

    def slot(k, g):
        return lane8 == (16 * row8 + 2 * k + g if g is not None else 16 * k + 12)

    for k in range(6):
        re, im = mom[2 * k], mom[2 * k + 1]
        both = jnp.where(apart, re, re + im)
        for g, x in ((c, both), (None, im)):
            big = 256.0 * jnp.max(x, axis=1, keepdims=True)
            hi = (x + big) - big
            lo = x - hi
            where = slot(k, g) if g is not None else slot(k, g) & apart
            packed[0] = jnp.where(where, jnp.sum(hi, axis=1, keepdims=True), packed[0])
            packed[1] = jnp.where(where, jnp.sum(lo, axis=1, keepdims=True), packed[1])
    mine = jnp.concatenate([jnp.sum(x, axis=0, keepdims=True) for x in packed], axis=1)
    ar_send[...] = mine
    ar_all[me] = mine

    def tell(k):
        return pltpu.make_async_remote_copy(
            src_ref=ar_send,
            dst_ref=ar_all.at[me],
            send_sem=m_send.at[k],
            recv_sem=m_recv.at[me],
            device_id=pos(lax.rem(me + k, total)),
            device_id_type=MESH,
        )

    def tell_one(k, carry):
        tell(k).start()
        return carry

    lax.fori_loop(1, total, tell_one, 0)

    def told(k, carry):
        source = lax.rem(me + k, total)
        pltpu.make_async_remote_copy(
            src_ref=ar_send,
            dst_ref=ar_all.at[source],
            send_sem=m_send.at[k],
            recv_sem=m_recv.at[source],
            device_id=pos(source),
            device_id_type=MESH,
        ).wait_recv()
        return carry

    lax.fori_loop(1, total, told, 0)
    sums = [(ar_all[i][:, 0:128], ar_all[i][:, 128:256]) for i in range(total)]
    while len(sums) > 1:
        sums = [pair_add(sums[2 * i], sums[2 * i + 1]) for i in range(len(sums) // 2)]
    whole = [jnp.broadcast_to(x, (8, 128)) for x in sums[0]]
    mu = []
    for k in range(6):
        sides = []
        for x in whole:
            groups = [
                jnp.broadcast_to(
                    jnp.sum(jnp.where(slot(k, g), x, 0.0), axis=1, keepdims=True), (8, 128)
                )
                for g in (0, 1, None)
            ]
            sides.append(jnp.concatenate(groups, axis=0))
        mu.append(tuple(sides))
    for k, w in enumerate(krylov_weights(mu)):
        coef[k, 0] = w[0:pairs]
        coef[k, 1] = jnp.where(row16 == 0, w[pairs : pairs + 1], w[0:pairs])

    def given(q, carry):
        pltpu.make_async_remote_copy(
            src_ref=basis.at[2, :, pl.ds(2 * q, 2)],
            dst_ref=basis.at[1 - c, :, pl.ds(2 * q, 2)],
            send_sem=y_send.at[q],
            recv_sem=y_recv.at[q],
            device_id=partner,
            device_id_type=MESH,
        ).wait_recv()
        return carry

    lax.fori_loop(0, share, given, 0)

    def restore(p, carry):
        r = pl.multiple_of((p // tiles) * 8, 8)
        q = pl.multiple_of(lax.rem(p, tiles) * 128, 128)
        here = (pl.ds(r, 8), pl.ds(q, 128))

        def field(j, part):
            terms = [
                coef[k, part, j : j + 1, :] * basis[(j // share, k, 2 * (j % share) + part) + here]
                for k in range(3)
            ]
            return terms[0] + terms[1] + terms[2]

        freq = [(field(0, 0), None)]
        freq += [(field(j, 0), field(j, 1)) for j in range(1, pairs)]
        freq += [(field(0, 1), None)]
        for n, x in enumerate(irfft_list(freq)):
            corr[n, pl.ds(r, 8), pl.ds(q, 128)] = x * tab[length + n]
        return carry

    lax.fori_loop(0, row_tiles * tiles, restore, 0)

    def block_of(source, core):
        return pl.multiple_of(lax.rem(source, half) * slab + piece * core, 8)

    def returning(dest):
        return pltpu.make_async_remote_copy(
            src_ref=corr.at[pl.ds(2 * dest, 2)],
            dst_ref=back.at[:, pl.ds(block_of(t, c), piece)],
            send_sem=b_send.at[dest],
            recv_sem=b_recv.at[place, c],
            device_id={"tm": dest, "rows": home},
            device_id_type=MESH,
        )

    def send_back(k, carry):
        returning(peer(k)).start()
        return carry

    lax.fori_loop(0, count - 1, send_back, 0)

    @pl.when(home != c)
    def _():
        returning(t).start()

    sq_copy.wait()
    rms = jnp.sqrt(
        jnp.sum(jnp.sum(sq_send[...] + sq_recv[...], axis=2, keepdims=True), axis=1, keepdims=True) / cells
        + rms_eps
    )
    rms_ref[...] = jnp.broadcast_to(rms[:, 0], (2, 128))

    def final(source, core, piece_of):
        start = block_of(source, core)
        ahead = pl.ds(pl.multiple_of(start + 8, 8), piece)
        out_ref[:, pl.ds(start, piece), :] = u_ext[:, ahead, :] + piece_of

    @pl.when(home == c)
    def _():
        final(t, c, corr[pl.ds(2 * t, 2)])

    def returned(j, carry):
        source = chip(j)
        for core in (0, 1):

            @pl.when(elsewhere(source, core))
            def _():
                block = pl.ds(block_of(source, core), piece)
                pltpu.make_async_remote_copy(
                    src_ref=corr.at[pl.ds(0, 2)],
                    dst_ref=back.at[:, block],
                    send_sem=b_send.at[0],
                    recv_sem=b_recv.at[lax.rem(source, half), core],
                    device_id={"tm": source},
                    device_id_type=MESH,
                ).wait_recv()
                final(source, core, back[:, block, :])

        return carry

    lax.fori_loop(0, half, returned, 0)

    for rim in rims:
        rim.wait_send()

    @pl.when(t < count - 1)
    def _():
        onward.wait_send()

    def drain_forward(j, carry):
        dest = chip(j)
        for core in (0, 1):

            @pl.when(elsewhere(dest, core))
            def _():
                forward(0, dest, core).wait_send()

            @pl.when(elsewhere(dest, core) & (dest != across))
            def _():
                forward(1, dest, core).wait_send()

        return carry

    lax.fori_loop(0, half, drain_forward, 0)

    @pl.when(home != c)
    def _():
        hop.wait_send()

    @pl.when(relays)
    def _():
        hop_on(0).wait_send()
        hop_on(1).wait_send()

    def drain_back(k, carry):
        returning(peer(k)).wait_send()
        return carry

    lax.fori_loop(0, count - 1, drain_back, 0)

    @pl.when(home != c)
    def _():
        returning(t).wait_send()

    def drain_pairs(q, carry):
        halo(0, q).wait_send()
        halo(1, q).wait_send()
        swap(q).wait_send()
        give(q).wait_send()
        return carry

    lax.fori_loop(0, share, drain_pairs, 0)

    def drain_tell(k, carry):
        tell(k).wait_send()
        return carry

    lax.fori_loop(1, total, drain_tell, 0)


def tables(length):
    pairs = length // 2
    n = np.arange(length)
    growth = np.exp(np.log(circulant_alpha) * n / length)
    root = np.exp(np.log(circulant_alpha) / length)
    j = np.arange(pairs)
    a_re = 1.0 - root * np.cos(2.0 * np.pi * j / length)
    a_im = a_re.copy()
    a_im[0] = 1.0 + root
    b = root * np.sin(2.0 * np.pi * j / length)
    return np.concatenate([growth, 1.0 / (length * growth), a_re, a_im, b]).astype(np.float32)


def shards(iterate, forcing, initial_state, diffusivity):
    steps, rows, cols = iterate.shape
    count = lax.axis_size("tm")
    halves = lax.axis_size("rows")
    length = steps * count
    assert steps == 2 and halves == 2
    slab = 2 * rows // count
    pairs = length // 2
    share = pairs // 2
    cells = rows * halves * cols
    f32 = jnp.float32
    vmem = pltpu.VMEM
    dma = pltpu.SemaphoreType.DMA
    hbm = pl.BlockSpec(memory_space=pl.ANY)
    updated, rms = pl.pallas_call(
        functools.partial(kernel, count, cells),
        out_shape=(
            vmem((steps, rows, cols), f32),
            vmem((steps, 128), f32),
        ),
        in_specs=[hbm] * 4 + [pl.BlockSpec(memory_space=pltpu.SMEM)],
        out_specs=(pl.BlockSpec(memory_space=vmem), pl.BlockSpec(memory_space=vmem)),
        scratch_shapes=[
            vmem((steps, rows + 16, cols), f32),
            vmem((steps, rows, cols), f32),
            vmem((rows, cols), f32),
            vmem((2 * rows + 32, cols), f32),
            vmem((steps, rows, cols), f32),
            vmem((length, slab // 2, cols), f32),
            vmem((slab, cols), f32),
            vmem((2, pairs, slab + 16, cols), f32),
            vmem((3, 3, pairs, slab // 2, cols), f32),
            vmem((length, slab // 2, cols), f32),
            vmem((steps, rows, cols), f32),
            vmem((5, slab + 16, cols), f32),
            vmem((2, cols // 128, slab + 32, 128), f32),
            vmem((12, share, 128), f32),
            vmem((3, 2, pairs, 128), f32),
            vmem((1, 256), f32),
            vmem((2 * count, 1, 256), f32),
            vmem((2, 8, 128), f32),
            vmem((2, 8, 128), f32),
            dma((3,)),
            dma((3,)),
            dma((4,)),
            dma((3,)),
            dma((3,)),
            dma((2, count // 2, 2)),
            dma((2, count)),
            dma((2, share)),
            dma((2, share)),
            dma((share,)),
            dma((share,)),
            dma((share,)),
            dma((share,)),
            dma((2 * count,)),
            dma((2 * count,)),
            dma((count,)),
            dma((count // 2, 2)),
            pltpu.SemaphoreType.REGULAR,
            pltpu.SemaphoreType.REGULAR,
        ],
        compiler_params=pltpu.CompilerParams(collective_id=0, has_side_effects=True),
        name="paradiag",
    )(iterate, forcing, initial_state, diffusivity, jnp.asarray(tables(length)))
    return updated, rms[:, 0]


def solution(mesh):
    placed = (
        P(("groups", "tm"), "rows", None),
        P(("groups", "tm"), "rows", None),
        P(("groups", "rows"), None),
        P(("groups", "rows"), None),
    )
    return jax.shard_map(
        shards,
        mesh=mesh,
        in_specs=placed,
        out_specs=(P(("groups", "tm"), "rows", None), P(("groups", "tm"))),
        check_vma=False,
    )
```

```python
import functools

import jax
import jax.numpy as jnp
import numpy as np
from jax import lax
from jax.experimental import pallas as pl
from jax.experimental.pallas import tpu as pltpu
from jax.sharding import PartitionSpec as P

circulant_alpha = 0.05
time_step = 0.5
rms_eps = 1e-06
MESH = pl.DeviceIdType.MESH


def rfft_list(x):
    n = len(x)
    if n == 1:
        return [(x[0], None)]
    even, odd = rfft_list(x[0::2]), rfft_list(x[1::2])
    half = n // 2
    out = [None] * (half + 1)
    out[0] = (even[0][0] + odd[0][0], None)
    out[half] = (even[0][0] - odd[0][0], None)
    for k in range(1, half // 2 + 1):
        if 2 * k == half:
            out[k] = (even[k][0], -odd[k][0])
            continue
        angle = 2.0 * np.pi * k / n
        cos, sin = float(np.cos(angle)), float(np.sin(angle))
        o_re, o_im = odd[k]
        if 8 * k == n:
            t_re, t_im = (o_re + o_im) * cos, (o_im - o_re) * cos
        else:
            t_re, t_im = o_re * cos + o_im * sin, o_im * cos - o_re * sin
        e_re, e_im = even[k]
        out[k] = (e_re + t_re, e_im + t_im)
        out[half - k] = (e_re - t_re, t_im - e_im)
    return out


def irfft_list(freq):
    half = len(freq) - 1
    n = 2 * half
    if n == 2:
        return [freq[0][0] + freq[1][0], freq[0][0] - freq[1][0]]
    even, odd = [None] * (half // 2 + 1), [None] * (half // 2 + 1)
    even[0] = (freq[0][0] + freq[half][0], None)
    odd[0] = (freq[0][0] - freq[half][0], None)
    for k in range(1, half // 2 + 1):
        if 2 * k == half:
            even[k] = (freq[k][0] + freq[k][0], None)
            odd[k] = (-(freq[k][1] + freq[k][1]), None)
            continue
        angle = 2.0 * np.pi * k / n
        cos, sin = float(np.cos(angle)), float(np.sin(angle))
        a_re, a_im = freq[k]
        b_re, b_im = freq[half - k]
        even[k] = (a_re + b_re, a_im - b_im)
        d_re, d_im = a_re - b_re, a_im + b_im
        if 8 * k == n:
            odd[k] = ((d_re - d_im) * cos, (d_re + d_im) * cos)
        else:
            odd[k] = (d_re * cos - d_im * sin, d_im * cos + d_re * sin)
    even_out, odd_out = irfft_list(even), irfft_list(odd)
    out = [None] * n
    out[0::2], out[1::2] = even_out, odd_out
    return out


def two_sum(a, b):
    s = a + b
    v = s - a
    return s, (a - (s - v)) + (b - v)


def quick_sum(a, b):
    s = a + b
    return s, b - (s - a)


def split(a):
    t = 4097.0 * a
    hi = t - (t - a)
    return hi, a - hi


def two_prod(a, b):
    p = a * b
    ah, al = split(a)
    bh, bl = split(b)
    return p, ((ah * bh - p) + ah * bl + al * bh) + al * bl


def pair_add(x, y):
    s, e = two_sum(x[0], y[0])
    return quick_sum(s, e + (x[1] + y[1]))


def pair_neg(x):
    return (-x[0], -x[1])


def pair_mul(x, y):
    p, e = two_prod(x[0], y[0])
    return quick_sum(p, e + (x[0] * y[1] + x[1] * y[0]))


def pair_div(x, y):
    q = x[0] / y[0]
    rest = pair_add(x, pair_neg(pair_mul((q, jnp.zeros_like(q)), y)))
    return quick_sum(q, rest[0] / y[0])


def krylov_weights(mu):
    one = (jnp.ones_like(mu[0][0]), jnp.zeros_like(mu[0][0]))
    zero = jnp.zeros_like(mu[0][0])
    inv0 = pair_div(one, mu[0])
    t1 = pair_div(mu[0], mu[1])
    t2 = pair_mul(t1, t1)
    t3 = pair_mul(t2, t1)
    t4 = pair_mul(t2, t2)
    t5 = pair_mul(t4, t1)
    m2, m3, m4, m5 = (
        pair_mul(pair_mul(mu[k], inv0), t) for k, t in ((2, t2), (3, t3), (4, t4), (5, t5))
    )
    tiny = 2.0**-32
    gain0 = pair_add(m2, pair_neg(one))
    den1 = pair_add(m3, pair_neg(pair_mul(m2, m2)))
    ok1 = (gain0[0] > tiny) & (den1[0] > tiny * m3[0])

    def kept(ok, x, other):
        return (jnp.where(ok, x[0], other), jnp.where(ok, x[1], 0.0))

    rate1 = kept(ok1, pair_div(kept(ok1, gain0, 0.0), kept(ok1, den1, 1.0)), 0.0)
    mid = pair_add(one, pair_mul(rate1, m2))
    inner = pair_add(pair_add(m2, pair_neg(pair_mul(mid, m3))), pair_mul(rate1, m4))
    size = m2[0] + mid[0] * m3[0] + rate1[0] * m4[0]
    ok2 = ok1 & (inner[0] > tiny * size)
    gamma2 = pair_mul(rate1, kept(ok2, inner, 0.0))
    gain1 = pair_div(gamma2, kept(ok1, gain0, 1.0))
    base = pair_add(one, pair_mul(gain1, m2))
    slope = pair_add(mid, gain1)
    inner2 = pair_add(
        pair_add(pair_mul(base, m3), pair_neg(pair_mul(slope, m4))), pair_mul(rate1, m5)
    )
    size2 = base[0] * m3[0] + slope[0] * m4[0] + rate1[0] * m5[0]
    ok3 = ok2 & (inner2[0] > tiny * size2)
    ratio = kept(ok2, inner, 0.0)
    rate2 = pair_div(ratio, kept(ok3, inner2, 1.0))
    rate2 = jnp.where(ok3, rate2[0], zero)
    w0 = mid[0] + rate2 * base[0]
    w1 = -(rate1[0] + rate2 * slope[0])
    w2 = rate2 * rate1[0]
    return w0 * t1[0], w1 * t2[0], w2 * t3[0]


def kernel(
    count,
    cells,
    it_hbm,
    fo_hbm,
    init_hbm,
    di_hbm,
    tab,
    out_ref,
    rms_ref,
    u_ext,
    force,
    before,
    d_ext,
    res,
    by_cell,
    stop,
    spec,
    basis,
    corr,
    back,
    weights,
    lined,
    mom,
    coef,
    ar_send,
    ar_all,
    sq_send,
    sq_recv,
    load_sem,
    prev_sem,
    hop_sem,
    rim_send,
    rim_recv,
    a_send,
    a_recv,
    h_send,
    h_recv,
    x_send,
    x_recv,
    y_send,
    y_recv,
    m_send,
    m_recv,
    b_send,
    b_recv,
    from_left,
    from_right,
):
    t = lax.axis_index("tm")
    c = lax.axis_index("rows")
    me = c * count + t
    total = 2 * count
    length = 2 * count
    pairs = length // 2
    share = pairs // 2
    rows = force.shape[1]
    cols = force.shape[2]
    half = count // 2
    slab = rows // half
    piece = slab // 2
    tiles = cols // 128
    home = t // half
    place = lax.rem(t, half)

    def pos(i):
        return {"tm": lax.rem(i, count), "rows": i // count}

    barrier = pltpu.get_barrier_semaphore()

    right, left = {"tm": lax.rem(t + 1, count)}, {"tm": lax.rem(t + count - 1, count)}
    partner = {"rows": 1 - c}
    for neighbour in (left, right, partner):
        pl.semaphore_signal(barrier, inc=1, device_id=neighbour, device_id_type=MESH)

    loads = [
        pltpu.make_async_copy(di_hbm, d_ext.at[pl.ds(pl.multiple_of(16 + rows * c, 8), rows)], load_sem.at[0]),
        pltpu.make_async_copy(it_hbm, u_ext.at[:, pl.ds(8, rows)], load_sem.at[1]),
        pltpu.make_async_copy(fo_hbm, force, load_sem.at[2]),
    ]
    for load in loads:
        load.start()
    u_ext[:, pl.ds(pl.multiple_of(c * (rows + 8), 8), 8), :] = jnp.zeros((2, 8, cols), jnp.float32)
    pl.semaphore_wait(barrier, 3)

    onward = pltpu.make_async_remote_copy(
        src_ref=it_hbm.at[1],
        dst_ref=before,
        send_sem=prev_sem.at[0],
        recv_sem=prev_sem.at[1],
        device_id=right,
        device_id_type=MESH,
    )
    first = pltpu.make_async_copy(init_hbm, before, prev_sem.at[2])

    @pl.when(t < count - 1)
    def _():
        onward.start()

    @pl.when(t == 0)
    def _():
        first.start()

    rims = [
        pltpu.make_async_remote_copy(
            src_ref=di_hbm,
            dst_ref=d_ext.at[pl.ds(pl.multiple_of(16 + rows * c, 8), rows)],
            send_sem=rim_send.at[0],
            recv_sem=rim_recv.at[0],
            device_id=partner,
            device_id_type=MESH,
        ),
        pltpu.make_async_remote_copy(
            src_ref=it_hbm.at[:, pl.ds(pl.multiple_of((1 - c) * (rows - 8), 8), 8)],
            dst_ref=u_ext.at[:, pl.ds(pl.multiple_of(c * (rows + 8), 8), 8)],
            send_sem=rim_send.at[1],
            recv_sem=rim_recv.at[1],
            device_id=partner,
            device_id_type=MESH,
        ),
    ]
    for rim in rims:
        rim.start()

    for load in loads:
        load.wait()
    for rim in rims:
        rim.wait_recv()
    d_ext[0:16, :] = jnp.broadcast_to(d_ext[16:24, :][:1], (16, cols))
    last = 2 * rows + 16
    d_ext[last : last + 16, :] = jnp.broadcast_to(d_ext[last - 8 : last, :][7:8], (16, cols))

    def lane_of(shape):
        return lax.broadcasted_iota(jnp.int32, shape, 1)

    def residual(step, start):
        tall = slab + 16
        u = u_ext[step, pl.ds(start, tall), :]
        d = d_ext[pl.ds(pl.multiple_of(rows * c + start + 8, 8), tall), :]
        lane = lane_of((slab, cols))
        mid = slice(8, slab + 8)
        uc, dc = u[mid], d[mid]
        u_n, u_s = pltpu.roll(u, 1, 0)[mid], pltpu.roll(u, tall - 1, 0)[mid]
        d_n, d_s = pltpu.roll(d, 1, 0)[mid], pltpu.roll(d, tall - 1, 0)[mid]
        u_w = jnp.where(lane == 0, 0.0, pltpu.roll(uc, 1, 1))
        u_e = jnp.where(lane == cols - 1, 0.0, pltpu.roll(uc, cols - 1, 1))
        d_w = jnp.where(lane == 0, dc, pltpu.roll(dc, 1, 1))
        d_e = jnp.where(lane == cols - 1, dc, pltpu.roll(dc, cols - 1, 1))
        spread = (
            (dc + d_n) * (uc - u_n)
            + (dc + d_s) * (uc - u_s)
            + (dc + d_w) * (uc - u_w)
            + (dc + d_e) * (uc - u_e)
        )
        if step == 0:
            prev = before[pl.ds(start, slab), :]
        else:
            prev = u_ext[step - 1, pl.ds(pl.multiple_of(start + 8, 8), slab), :]
        value = time_step * force[step, pl.ds(start, slab), :] + prev - uc
        return value - (0.5 * time_step) * spread

    def squares(value):
        sq = value * value
        folded = sq[0:8]
        for i in range(1, slab // 8):
            folded = folded + sq[8 * i : 8 * i + 8]
        total_sq = folded[:, 0:128]
        for i in range(1, tiles):
            total_sq = total_sq + folded[:, 128 * i : 128 * i + 128]
        return total_sq

    def forward(step, dest, core):
        start = pl.multiple_of(lax.rem(dest, half) * slab + piece * core, 8)
        return pltpu.make_async_remote_copy(
            src_ref=res.at[step, pl.ds(start, piece)],
            dst_ref=by_cell.at[2 * t + step],
            send_sem=a_send.at[step, lax.rem(dest, half), core],
            recv_sem=a_recv.at[step, t],
            device_id={"tm": dest, "rows": core},
            device_id_type=MESH,
        )

    def chip(j):
        return half * c + lax.rem(t + half // 2 + j, half)

    def elsewhere(dest, core):
        return jnp.logical_or(dest != t, core != c)

    def peer(k):
        far = count // 2 - (k + 1) // 2
        return lax.rem(t + jnp.where(lax.rem(k, 2) == 1, far, count - far), count)

    def make(step, dest):
        start = pl.multiple_of(lax.rem(dest, half) * slab, slab)
        value = residual(step, start)
        res[step, pl.ds(start, slab), :] = value * tab[2 * t + step]
        sq_send[step] = sq_send[step] + squares(value)

    def send_one(step, dest):
        @pl.when(dest // half == c)
        def _():
            make(step, dest)
            forward(step, dest, 0).start()
            forward(step, dest, 1).start()

    def send_home(step):
        @pl.when(home == c)
        def _():
            make(step, t)
            start = pl.multiple_of(place * slab + piece * c, 8)
            by_cell[2 * t + step] = res[step, pl.ds(start, piece), :]
            forward(step, t, 1 - c).start()

    across = lax.rem(t + half, count)
    hop = pltpu.make_async_remote_copy(
        src_ref=res.at[1, pl.ds(pl.multiple_of(lax.rem(across, half) * slab, slab), slab)],
        dst_ref=stop,
        send_sem=hop_sem.at[0],
        recv_sem=hop_sem.at[1],
        device_id={"tm": lax.rem(t + count - half // 2, count)},
        device_id_type=MESH,
    )
    origin = lax.rem(t + half // 2, count)
    relays = lax.rem(origin + half, count) // half == c

    def hop_on(core):
        return pltpu.make_async_remote_copy(
            src_ref=stop.at[pl.ds(piece * core, piece)],
            dst_ref=by_cell.at[2 * origin + 1],
            send_sem=hop_sem.at[2 + core],
            recv_sem=a_recv.at[1, origin],
            device_id={"tm": lax.rem(t + count - half // 2, count), "rows": core},
            device_id_type=MESH,
        )

    def widen(k, carry):
        pl.semaphore_signal(from_left, inc=1, device_id=right, device_id_type=MESH)
        pl.semaphore_signal(from_right, inc=1, device_id=left, device_id_type=MESH)
        pl.semaphore_wait(from_left, 1)
        pl.semaphore_wait(from_right, 1)
        @pl.when(k < half)
        def _():
            send_one(1, lax.rem(t + k, count))
            send_one(1, lax.rem(t + count - k, count))

        @pl.when((k == half // 2) & (home != c))
        def _():
            make(1, across)
            hop.start()

        return carry

    sq_send[...] = jnp.zeros((2, 8, 128), jnp.float32)
    lax.fori_loop(1, half + 1, widen, 0)
    send_home(1)

    @pl.when(relays)
    def _():
        hop.wait_recv()
        hop_on(0).start()
        hop_on(1).start()

    @pl.when(t > 0)
    def _():
        onward.wait_recv()

    @pl.when(t == 0)
    def _():
        first.wait()

    def send_far(k, carry):
        send_one(0, peer(k))
        return carry

    lax.fori_loop(0, count - 1, send_far, 0)
    send_home(0)

    sq_copy = pltpu.make_async_remote_copy(
        src_ref=sq_send,
        dst_ref=sq_recv,
        send_sem=rim_send.at[2],
        recv_sem=rim_recv.at[2],
        device_id=partner,
        device_id_type=MESH,
    )
    sq_copy.start()

    d = d_ext[pl.ds(pl.multiple_of(t * slab, slab), slab + 32), :]
    tall = slab + 16
    mid = slice(8, slab + 24)
    dc = d[mid]
    lane = lane_of((tall, cols))
    line = lax.broadcasted_iota(jnp.int32, (tall, cols), 0)
    outside = ((t == 0) & (line < 8)) | ((t == count - 1) & (line >= slab + 8))
    quarter = 0.5 * time_step
    w_n = quarter * (dc + pltpu.roll(d, 1, 0)[mid])
    w_s = quarter * (dc + pltpu.roll(d, slab + 31, 0)[mid])
    w_w = quarter * (dc + jnp.where(lane == 0, dc, pltpu.roll(dc, 1, 1)))
    w_e = quarter * (dc + jnp.where(lane == cols - 1, dc, pltpu.roll(dc, cols - 1, 1)))
    weights[0] = w_n + w_s + w_w + w_e
    weights[1] = jnp.where(outside, 0.0, w_n)
    weights[2] = jnp.where(outside, 0.0, w_s)
    weights[3] = jnp.where(lane == 0, 0.0, w_w)
    weights[4] = jnp.where(lane == cols - 1, 0.0, w_e)

    def arrival(step, source):
        return pltpu.make_async_remote_copy(
            src_ref=res.at[step, pl.ds(0, piece)],
            dst_ref=by_cell.at[2 * source + step],
            send_sem=a_send.at[step, 0, 0],
            recv_sem=a_recv.at[step, source],
            device_id={"tm": source},
            device_id_type=MESH,
        )

    def arrived(k, carry):
        for step in (0, 1):
            arrival(step, lax.rem(t + k, count)).wait_recv()
        return carry

    lax.fori_loop(1, count, arrived, 0)

    @pl.when(home != c)
    def _():
        for step in (0, 1):
            arrival(step, t).wait_recv()

    row_tiles = piece // 8

    def transform(p, carry):
        r = pl.multiple_of(lax.rem(p // tiles + c, row_tiles) * 8, 8)
        q = pl.multiple_of(lax.rem(p, tiles) * 128, 128)
        x = [by_cell[n, pl.ds(r, 8), pl.ds(q, 128)] for n in range(length)]
        f = rfft_list(x)
        here = (pl.ds(pl.multiple_of(r + 8 + piece * c, 8), 8), pl.ds(q, 128))
        spec[(0, 0) + here] = f[0][0]
        spec[(0, 1) + here] = f[pairs][0]
        for j in range(1, pairs):
            for part in (0, 1):
                spec[(j // share, 2 * (j % share) + part) + here] = f[j][part]
        return carry

    lax.fori_loop(0, tiles, transform, 0)

    beyond = {"tm": lax.rem(t + count + 2 * c - 1, count)}
    src_edge = pl.ds(pl.multiple_of(8 + (slab - 8) * c, 8), 8)
    dst_edge = pl.ds(pl.multiple_of((slab + 8) * (1 - c), 8), 8)

    def halo(group, q):
        fields = pl.ds(2 * q, 2)
        return pltpu.make_async_remote_copy(
            src_ref=spec.at[group, fields, src_edge],
            dst_ref=spec.at[group, fields, dst_edge],
            send_sem=h_send.at[group, q],
            recv_sem=h_recv.at[1 - c, q],
            device_id={**beyond, "rows": group},
            device_id_type=MESH,
        )

    own_part = pl.ds(pl.multiple_of(8 + piece * c, 8), piece)

    def swap(q):
        fields = pl.ds(2 * q, 2)
        return pltpu.make_async_remote_copy(
            src_ref=spec.at[1 - c, fields, own_part],
            dst_ref=spec.at[1 - c, fields, own_part],
            send_sem=x_send.at[q],
            recv_sem=x_recv.at[q],
            device_id=partner,
            device_id_type=MESH,
        )

    def send_halo(q, carry):
        halo(0, q).start()
        halo(1, q).start()
        return carry

    def send_swap(q, carry):
        swap(q).start()
        return carry

    lax.fori_loop(0, share, send_halo, 0)
    lax.fori_loop(tiles, row_tiles * tiles, transform, 0)
    lax.fori_loop(0, share, send_swap, 0)

    top = jnp.where(t == 0, 0.0, 1.0)
    bottom = jnp.where(t == count - 1, 0.0, 1.0)
    n_tr = slab // 8 + 2

    def spread_of(v, wanted, shift, part):
        for i in range(n_tr):
            for k in range(tiles):
                lined[part, k, 8 * i + 8 : 8 * i + 16, :] = v[i][:, 128 * k : 128 * k + 128]
        out = {}
        for i in wanted:
            v_n, v_s = (
                jnp.concatenate(
                    [lined[part, k, 8 * i + 8 + o : 8 * i + 16 + o, :] for k in range(tiles)], axis=1
                )
                for o in (-1, 1)
            )
            here = slice(8 * i, 8 * i + 8)
            out[i] = (
                (weights[0, here, :] + shift) * v[i]
                - weights[1, here, :] * v_n
                - weights[2, here, :] * v_s
                - weights[3, here, :] * pltpu.roll(v[i], 1, 1)
                - weights[4, here, :] * pltpu.roll(v[i], cols - 1, 1)
            )
        return out

    def clip(i, x):
        if i == 0:
            return x * top
        if i == n_tr - 1:
            return x * bottom
        return x

    inner = range(1, n_tr - 1)

    def folded(v):
        acc = None
        for i in inner:
            sq = v[i] * v[i]
            for k in range(tiles):
                part = sq[:, 128 * k : 128 * k + 128]
                acc = part if acc is None else acc + part
        return jnp.sum(acc, axis=0, keepdims=True)

    def give(q):
        return pltpu.make_async_remote_copy(
            src_ref=basis.at[2, :, pl.ds(2 * q, 2)],
            dst_ref=basis.at[c, :, pl.ds(2 * q, 2)],
            send_sem=y_send.at[q],
            recv_sem=y_recv.at[q],
            device_id=partner,
            device_id_type=MESH,
        )

    def solve(q, carry):
        for side in (0, 1):
            pltpu.make_async_remote_copy(
                src_ref=spec.at[c, pl.ds(2 * q, 2), src_edge],
                dst_ref=spec.at[c, pl.ds(2 * q, 2), pl.ds((slab + 8) * side, 8)],
                send_sem=h_send.at[0, q],
                recv_sem=h_recv.at[side, q],
                device_id=partner,
                device_id_type=MESH,
            ).wait_recv()
        pltpu.make_async_remote_copy(
            src_ref=spec.at[c, pl.ds(2 * q, 2), own_part],
            dst_ref=spec.at[c, pl.ds(2 * q, 2), pl.ds(pl.multiple_of(8 + piece * (1 - c), 8), piece)],
            send_sem=x_send.at[q],
            recv_sem=x_recv.at[q],
            device_id=partner,
            device_id_type=MESH,
        ).wait_recv()
        j = 2 * length + share * c + q
        a_re, a_im, b = tab[j], tab[j + pairs], tab[j + 2 * pairs]
        v = [
            [clip(i, spec[c, 2 * q + part, 8 * i : 8 * i + 8, :]) for i in range(n_tr)]
            for part in (0, 1)
        ]
        for order in range(6):
            wanted = inner if order == 5 else range(n_tr)
            sign = b if order % 2 == 0 else -b
            k_re, k_im = spread_of(v[0], wanted, a_re, 0), spread_of(v[1], wanted, a_im, 1)
            new_re, new_im = [None] * n_tr, [None] * n_tr
            for i in wanted:
                new_re[i] = sign * v[1][i] + k_re[i]
                new_im[i] = k_im[i] - sign * v[0][i]
            v = [new_re, new_im]
            mom[2 * order, pl.ds(q, 1), :] = folded(v[0])
            mom[2 * order + 1, pl.ds(q, 1), :] = folded(v[1])
            if order % 2 == 0:
                for part in (0, 1):
                    for i in inner:
                        line = (8 * i - 8) % piece
                        keep = 2 * c if 8 * i - 8 < piece else 2 - c
                        basis[keep, order // 2, 2 * q + part, line : line + 8, :] = v[part][i]
        give(q).start()
        return carry

    lined[...] = jnp.zeros(lined.shape, jnp.float32)
    lax.fori_loop(0, share, solve, 0)

    lane8 = lax.broadcasted_iota(jnp.int32, (8, 128), 1)
    row8 = lax.broadcasted_iota(jnp.int32, (8, 128), 0)
    row16 = lax.broadcasted_iota(jnp.int32, (pairs, 128), 0)
    apart = (row8 == 0) & (c == 0)
    packed = [jnp.zeros((8, 128), jnp.float32), jnp.zeros((8, 128), jnp.float32)]

    def slot(k, g):
        return lane8 == (16 * row8 + 2 * k + g if g is not None else 16 * k + 12)

    for k in range(6):
        re, im = mom[2 * k], mom[2 * k + 1]
        both = jnp.where(apart, re, re + im)
        for g, x in ((c, both), (None, im)):
            big = 256.0 * jnp.max(x, axis=1, keepdims=True)
            hi = (x + big) - big
            lo = x - hi
            where = slot(k, g) if g is not None else slot(k, g) & apart
            packed[0] = jnp.where(where, jnp.sum(hi, axis=1, keepdims=True), packed[0])
            packed[1] = jnp.where(where, jnp.sum(lo, axis=1, keepdims=True), packed[1])
    mine = jnp.concatenate([jnp.sum(x, axis=0, keepdims=True) for x in packed], axis=1)
    ar_send[...] = mine
    ar_all[me] = mine

    def tell(k, dest, core):
        return pltpu.make_async_remote_copy(
            src_ref=ar_send,
            dst_ref=ar_all.at[me],
            send_sem=m_send.at[2 * k + core],
            recv_sem=m_recv.at[me],
            device_id={"tm": dest, "rows": core},
            device_id_type=MESH,
        )

    def tell_one(k, carry):
        dest = peer(k)
        tell(k, dest, 0).start()
        tell(k, dest, 1).start()
        return carry

    lax.fori_loop(0, count - 1, tell_one, 0)
    tell(count - 1, t, 1 - c).start()

    def told(k, carry):
        source = lax.rem(me + k, total)
        pltpu.make_async_remote_copy(
            src_ref=ar_send,
            dst_ref=ar_all.at[source],
            send_sem=m_send.at[k],
            recv_sem=m_recv.at[source],
            device_id=pos(source),
            device_id_type=MESH,
        ).wait_recv()
        return carry

    lax.fori_loop(1, total, told, 0)
    sums = [(ar_all[i][:, 0:128], ar_all[i][:, 128:256]) for i in range(total)]
    while len(sums) > 1:
        sums = [pair_add(sums[2 * i], sums[2 * i + 1]) for i in range(len(sums) // 2)]
    whole = [jnp.broadcast_to(x, (8, 128)) for x in sums[0]]
    mu = []
    for k in range(6):
        sides = []
        for x in whole:
            groups = [
                jnp.broadcast_to(
                    jnp.sum(jnp.where(slot(k, g), x, 0.0), axis=1, keepdims=True), (8, 128)
                )
                for g in (0, 1, None)
            ]
            sides.append(jnp.concatenate(groups, axis=0))
        mu.append(tuple(sides))
    for k, w in enumerate(krylov_weights(mu)):
        coef[k, 0] = w[0:pairs]
        coef[k, 1] = jnp.where(row16 == 0, w[pairs : pairs + 1], w[0:pairs])

    def given(q, carry):
        pltpu.make_async_remote_copy(
            src_ref=basis.at[2, :, pl.ds(2 * q, 2)],
            dst_ref=basis.at[1 - c, :, pl.ds(2 * q, 2)],
            send_sem=y_send.at[q],
            recv_sem=y_recv.at[q],
            device_id=partner,
            device_id_type=MESH,
        ).wait_recv()
        return carry

    lax.fori_loop(0, share, given, 0)

    def restore(p, carry):
        r = pl.multiple_of((p // tiles) * 8, 8)
        q = pl.multiple_of(lax.rem(p, tiles) * 128, 128)
        here = (pl.ds(r, 8), pl.ds(q, 128))

        def field(j, part):
            terms = [
                coef[k, part, j : j + 1, :] * basis[(j // share, k, 2 * (j % share) + part) + here]
                for k in range(3)
            ]
            return terms[0] + terms[1] + terms[2]

        freq = [(field(0, 0), None)]
        freq += [(field(j, 0), field(j, 1)) for j in range(1, pairs)]
        freq += [(field(0, 1), None)]
        for n, x in enumerate(irfft_list(freq)):
            corr[n, pl.ds(r, 8), pl.ds(q, 128)] = x * tab[length + n]
        return carry

    lax.fori_loop(0, row_tiles * tiles, restore, 0)

    def block_of(source, core):
        return pl.multiple_of(lax.rem(source, half) * slab + piece * core, 8)

    def returning(dest):
        return pltpu.make_async_remote_copy(
            src_ref=corr.at[pl.ds(2 * dest, 2)],
            dst_ref=back.at[:, pl.ds(block_of(t, c), piece)],
            send_sem=b_send.at[dest],
            recv_sem=b_recv.at[place, c],
            device_id={"tm": dest, "rows": home},
            device_id_type=MESH,
        )

    def send_back(k, carry):
        returning(peer(k)).start()
        return carry

    lax.fori_loop(0, count - 1, send_back, 0)

    @pl.when(home != c)
    def _():
        returning(t).start()

    sq_copy.wait()
    rms = jnp.sqrt(
        jnp.sum(jnp.sum(sq_send[...] + sq_recv[...], axis=2, keepdims=True), axis=1, keepdims=True) / cells
        + rms_eps
    )
    for i in range(2):
        rms_ref[i] = rms[i, 0, 0]

    def final(source, core, piece_of):
        start = block_of(source, core)
        ahead = pl.ds(pl.multiple_of(start + 8, 8), piece)
        out_ref[:, pl.ds(start, piece), :] = u_ext[:, ahead, :] + piece_of

    @pl.when(home == c)
    def _():
        final(t, c, corr[pl.ds(2 * t, 2)])

    def returned(j, carry):
        source = chip(j)
        for core in (0, 1):

            @pl.when(elsewhere(source, core))
            def _():
                block = pl.ds(block_of(source, core), piece)
                pltpu.make_async_remote_copy(
                    src_ref=corr.at[pl.ds(0, 2)],
                    dst_ref=back.at[:, block],
                    send_sem=b_send.at[0],
                    recv_sem=b_recv.at[lax.rem(source, half), core],
                    device_id={"tm": source},
                    device_id_type=MESH,
                ).wait_recv()
                final(source, core, back[:, block, :])

        return carry

    lax.fori_loop(0, half, returned, 0)

    for rim in rims:
        rim.wait_send()

    @pl.when(t < count - 1)
    def _():
        onward.wait_send()

    def drain_forward(j, carry):
        dest = chip(j)
        for core in (0, 1):

            @pl.when(elsewhere(dest, core))
            def _():
                forward(0, dest, core).wait_send()

            @pl.when(elsewhere(dest, core) & (dest != across))
            def _():
                forward(1, dest, core).wait_send()

        return carry

    lax.fori_loop(0, half, drain_forward, 0)

    @pl.when(home != c)
    def _():
        hop.wait_send()

    @pl.when(relays)
    def _():
        hop_on(0).wait_send()
        hop_on(1).wait_send()

    def drain_back(k, carry):
        returning(peer(k)).wait_send()
        return carry

    lax.fori_loop(0, count - 1, drain_back, 0)

    @pl.when(home != c)
    def _():
        returning(t).wait_send()

    def drain_pairs(q, carry):
        halo(0, q).wait_send()
        halo(1, q).wait_send()
        swap(q).wait_send()
        give(q).wait_send()
        return carry

    lax.fori_loop(0, share, drain_pairs, 0)

    def drain_tell(k, carry):
        dest = peer(k)
        tell(k, dest, 0).wait_send()
        tell(k, dest, 1).wait_send()
        return carry

    lax.fori_loop(0, count - 1, drain_tell, 0)
    tell(count - 1, t, 1 - c).wait_send()


def tables(length):
    pairs = length // 2
    n = np.arange(length)
    growth = np.exp(np.log(circulant_alpha) * n / length)
    root = np.exp(np.log(circulant_alpha) / length)
    j = np.arange(pairs)
    a_re = 1.0 - root * np.cos(2.0 * np.pi * j / length)
    a_im = a_re.copy()
    a_im[0] = 1.0 + root
    b = root * np.sin(2.0 * np.pi * j / length)
    return np.concatenate([growth, 1.0 / (length * growth), a_re, a_im, b]).astype(np.float32)


def shards(iterate, forcing, initial_state, diffusivity):
    steps, rows, cols = iterate.shape
    count = lax.axis_size("tm")
    halves = lax.axis_size("rows")
    length = steps * count
    assert steps == 2 and halves == 2
    slab = 2 * rows // count
    pairs = length // 2
    share = pairs // 2
    cells = rows * halves * cols
    f32 = jnp.float32
    vmem = pltpu.VMEM
    dma = pltpu.SemaphoreType.DMA
    hbm = pl.BlockSpec(memory_space=pl.ANY)
    updated, rms = pl.pallas_call(
        functools.partial(kernel, count, cells),
        out_shape=(
            vmem((steps, rows, cols), f32),
            jax.ShapeDtypeStruct((steps,), f32),
        ),
        in_specs=[hbm] * 4 + [pl.BlockSpec(memory_space=pltpu.SMEM)],
        out_specs=(pl.BlockSpec(memory_space=vmem), pl.BlockSpec(memory_space=pltpu.SMEM)),
        scratch_shapes=[
            vmem((steps, rows + 16, cols), f32),
            vmem((steps, rows, cols), f32),
            vmem((rows, cols), f32),
            vmem((2 * rows + 32, cols), f32),
            vmem((steps, rows, cols), f32),
            vmem((length, slab // 2, cols), f32),
            vmem((slab, cols), f32),
            vmem((2, pairs, slab + 16, cols), f32),
            vmem((3, 3, pairs, slab // 2, cols), f32),
            vmem((length, slab // 2, cols), f32),
            vmem((steps, rows, cols), f32),
            vmem((5, slab + 16, cols), f32),
            vmem((2, cols // 128, slab + 32, 128), f32),
            vmem((12, share, 128), f32),
            vmem((3, 2, pairs, 128), f32),
            vmem((1, 256), f32),
            vmem((2 * count, 1, 256), f32),
            vmem((2, 8, 128), f32),
            vmem((2, 8, 128), f32),
            dma((3,)),
            dma((3,)),
            dma((4,)),
            dma((3,)),
            dma((3,)),
            dma((2, count // 2, 2)),
            dma((2, count)),
            dma((2, share)),
            dma((2, share)),
            dma((share,)),
            dma((share,)),
            dma((share,)),
            dma((share,)),
            dma((2 * count,)),
            dma((2 * count,)),
            dma((count,)),
            dma((count // 2, 2)),
            pltpu.SemaphoreType.REGULAR,
            pltpu.SemaphoreType.REGULAR,
        ],
        compiler_params=pltpu.CompilerParams(collective_id=0, has_side_effects=True),
        name="paradiag",
    )(iterate, forcing, initial_state, diffusivity, jnp.asarray(tables(length)))
    return updated, rms


def solution(mesh):
    placed = (
        P(("groups", "tm"), "rows", None),
        P(("groups", "tm"), "rows", None),
        P(("groups", "rows"), None),
        P(("groups", "rows"), None),
    )
    return jax.shard_map(
        shards,
        mesh=mesh,
        in_specs=placed,
        out_specs=(P(("groups", "tm"), "rows", None), P(("groups", "tm"))),
        check_vma=False,
    )
```
